256 devices in a mesh: lat: 32 (over y_hi, z, core), ch: 8 (over y_lo, x).
Axes of the slice: x: 4, y: 4 (y_hi: 2, y_lo: 2; y = y_hi * 2 + y_lo), z: 8, core: 2. Of those that a mesh axis runs over, the one named last changes fastest.
Arguments:
- tokens: bfloat16 [32, 64, 138240], P(None, 'lat', 'ch'), may hold values from -60 to 60
- norm_gain: float32 [768], P('ch'), may hold values from 0.25 to 1.75
- norm_shift: float32 [768], P('ch'), may hold values from -1.5 to 1.5
- first_weight: float32 [2, 8, 96, 96], P(None, 'ch'), may hold values from -0.625 to 0.625
- first_bias: float32 [2, 8, 96], P(None, 'ch'), may hold values from -1.5 to 1.5
- second_weight: float32 [2, 8, 96, 96], P(None, 'ch'), may hold values from -0.625 to 0.625
- second_bias: float32 [2, 8, 96], P(None, 'ch'), may hold values from -1.5 to 1.5
- upstream: bfloat16 [32, 64, 138240], P(None, 'lat', 'ch'), may hold values from -6 to 6
Outputs:
- result: bfloat16 [32, 64, 138240], P(None, 'lat', 'ch')
- grad_tokens: bfloat16 [32, 64, 138240], P(None, 'lat', 'ch')
- grad_first_weight: float32 [2, 8, 96, 96], P(None, 'ch')
- grad_first_bias: float32 [2, 8, 96], P(None, 'ch')
- grad_second_weight: float32 [2, 8, 96, 96], P(None, 'ch')
- grad_second_bias: float32 [2, 8, 96], P(None, 'ch')
- grad_norm_gain: float32 [768], P('ch')
- grad_norm_shift: float32 [768], P('ch')
The draws below stay inside these ranges and needn't reach their ends.
All inputs are finite; a program needn't handle non-finite values.
Results may differ from the reference program's by a relative error of at most 0.0086.
Values may be sent and summed in bfloat16 or wider, within the bound.
A program may use at most 192 MiB of HBM per device.

```python
import math
import jax
import jax.numpy as jnp
from jax import lax

EMBED = 768
BLOCKS = 8
LON = 180
LAT_CELLS = 64
BATCH = 32
BLOCK = 96


def draw_tokens(key, part):
    base_key = jax.random.fold_in(key, 7)
    key_list = jax.random.split(base_key, 4)
    dims_shape = (BATCH, LAT_CELLS, LON, EMBED)
    channel_index = jnp.arange(EMBED, dtype=jnp.float32)
    channel_scale = 0.6 * jnp.exp(math.log(3.0) * channel_index / max(EMBED - 1, 1))
    channel_scale = channel_scale * jnp.exp(jax.random.uniform(key_list[0], (EMBED,), jnp.float32, math.log(0.5), math.log(2.0)))
    token_scale = jnp.exp(jax.random.uniform(key_list[1], (BATCH, LAT_CELLS, LON, 1), jnp.float32, math.log(0.3), math.log(3.0)))
    values = jnp.clip(jax.random.normal(key_list[3], dims_shape, jnp.float32), -5.0, 5.0)
    field_out = values * channel_scale * token_scale
    return jnp.transpose(field_out, (0, 1, 3, 2)).reshape(BATCH, LAT_CELLS, EMBED * LON).astype(jnp.bfloat16)


def level_of(stream_key, dims, shards, smallest, largest):
    def one(axis_at, blocks):
        draws = jax.random.uniform(jax.random.fold_in(jax.random.fold_in(stream_key, 6), axis_at), (blocks,), jnp.float32, smallest / len(shards), largest / len(shards))
        return jnp.repeat(jnp.exp(draws), dims[axis_at] // blocks).reshape((-1,) + (1,) * (len(dims) - axis_at - 1))

    level = one(*shards[0])
    for cut in shards[1:]:
        level = level * one(*cut)
    return level


def gaussian(stream_key, extent, spread, limit, cuts=(), held_as=jnp.bfloat16):
    values = jax.random.normal(stream_key, extent, jnp.float32) * spread
    if len(cuts) > 0:
        values = level_of(stream_key, extent, cuts, -0.22, 0.18) * values
    return jnp.clip(values, min=-limit, max=limit).astype(held_as)


def setup_inputs(seed: int = 0) -> dict:
    key_of = jax.random.split(jax.random.key(seed), 9)
    tokens = draw_tokens(jax.random.fold_in(key_of[8], 71), 0)
    norm_gain = jnp.clip(1.0 + 0.15 * jax.random.normal(key_of[1], (EMBED,), jnp.float32), 0.25, 1.75)
    norm_shift = gaussian(key_of[2], (EMBED,), 0.3, 1.5, ((0, 8),), jnp.float32)
    first_weight = gaussian(key_of[3], (2, BLOCKS, BLOCK, BLOCK), BLOCK ** -0.5, 0.625, ((1, 8),), jnp.float32)
    first_bias = gaussian(key_of[4], (2, BLOCKS, BLOCK), 0.3, 1.5, ((1, 8),), jnp.float32)
    second_weight = gaussian(key_of[5], (2, BLOCKS, BLOCK, BLOCK), BLOCK ** -0.5, 0.625, ((1, 8),), jnp.float32)
    second_bias = gaussian(key_of[6], (2, BLOCKS, BLOCK), 0.3, 1.5, ((1, 8),), jnp.float32)
    upstream = gaussian(key_of[7], (BATCH, LAT_CELLS, EMBED * LON), 1.0, 6.0, ((1, 32), (2, 8)))
    return dict(tokens=tokens, norm_gain=norm_gain, norm_shift=norm_shift, first_weight=first_weight, first_bias=first_bias, second_weight=second_weight, second_bias=second_bias, upstream=upstream)


layer_eps = 1e-05
shrink_level = 0.1
highest = lax.Precision.HIGHEST

def block_mix(values, matrix):
    return jnp.einsum('bhknc,ncd->bhknd', values, matrix, precision=highest)

def smooth_gelu(values):
    return 0.5 * values * (1.0 + jnp.tanh(math.sqrt(2.0 / math.pi) * (values + 0.044715 * values * values * values)))

def spectral_mlp(real_part, imag_part, params):
    first_weight, first_bias, second_weight, second_bias = params
    dims_shape = real_part.shape
    groups = first_weight.shape[1]
    block_width = first_weight.shape[2]
    real_part = real_part.reshape(dims_shape[:-1] + (groups, block_width))
    imag_part = imag_part.reshape(dims_shape[:-1] + (groups, block_width))
    hidden_real = smooth_gelu(block_mix(real_part, first_weight[0]) - block_mix(imag_part, first_weight[1]) + first_bias[0])
    hidden_imag = smooth_gelu(block_mix(imag_part, first_weight[0]) + block_mix(real_part, first_weight[1]) + first_bias[1])
    mixed_real = block_mix(hidden_real, second_weight[0]) - block_mix(hidden_imag, second_weight[1]) + second_bias[0]
    mixed_imag = block_mix(hidden_imag, second_weight[0]) + block_mix(hidden_real, second_weight[1]) + second_bias[1]
    mixed_real = mixed_real - shrink_level * jnp.tanh(mixed_real / shrink_level)
    mixed_imag = mixed_imag - shrink_level * jnp.tanh(mixed_imag / shrink_level)
    return (mixed_real.reshape(dims_shape), mixed_imag.reshape(dims_shape))

def spectral_filter(field_in, params):
    spectrum = jnp.fft.rfft2(field_in, axes=(1, 2), norm='ortho')
    mixed_real, mixed_imag = spectral_mlp(jnp.real(spectrum), jnp.imag(spectrum), params)
    return jnp.fft.irfft2(mixed_real + 1j * mixed_imag, s=(LAT_CELLS, LON), axes=(1, 2), norm='ortho')

def unmerge(sample):
    return jnp.transpose(sample.reshape(LAT_CELLS, EMBED, LON), (0, 2, 1))

def merge(field_in):
    return jnp.transpose(field_in, (0, 2, 1)).reshape(LAT_CELLS, EMBED * LON)

def reference(tokens, norm_gain, norm_shift, first_weight, first_bias, second_weight, second_bias, upstream):
    params = (first_weight, first_bias, second_weight, second_bias)
    initial = (jnp.zeros_like(first_weight), jnp.zeros_like(first_bias), jnp.zeros_like(second_weight), jnp.zeros_like(second_bias), jnp.zeros_like(norm_gain), jnp.zeros_like(norm_shift))

    def per_sample(carry, items):
        sample, cotangent = items
        as_float = unmerge(sample).astype(jnp.float32)[None]
        totals = lax.optimization_barrier(jnp.sum(as_float, axis=-1, keepdims=True))
        squares = lax.optimization_barrier(jnp.sum(as_float * as_float, axis=-1, keepdims=True))
        center = totals / EMBED
        variance = squares / EMBED - center * center
        inv_scale = lax.rsqrt(variance + layer_eps)
        standard = (as_float - center) * inv_scale
        normed = lax.optimization_barrier((standard * norm_gain + norm_shift).astype(jnp.bfloat16))
        normed_float = normed.astype(jnp.float32)
        filtered_float, pullback = jax.vjp(spectral_filter, normed_float, params)
        filtered = lax.optimization_barrier(filtered_float.astype(jnp.bfloat16))
        result = (as_float + normed_float + filtered.astype(jnp.float32)).astype(jnp.bfloat16)
        grad_out = unmerge(cotangent).astype(jnp.float32)[None]
        field_grad, param_grads = pullback(grad_out)
        spectral_grad = lax.optimization_barrier(field_grad.astype(jnp.bfloat16))
        normed_grad = grad_out + spectral_grad.astype(jnp.float32)
        gain_part = lax.optimization_barrier(jnp.sum(normed_grad * standard, axis=(0, 1, 2)))
        shift_part = lax.optimization_barrier(jnp.sum(normed_grad, axis=(0, 1, 2)))
        standard_grad = normed_grad * norm_gain
        grad_mean = lax.optimization_barrier(jnp.sum(standard_grad, axis=-1, keepdims=True)) / EMBED
        grad_cross = lax.optimization_barrier(jnp.sum(standard_grad * standard, axis=-1, keepdims=True)) / EMBED
        grad_tokens = (grad_out + inv_scale * (standard_grad - grad_mean - standard * grad_cross)).astype(jnp.bfloat16)
        updated = (carry[0] + param_grads[0], carry[1] + param_grads[1], carry[2] + param_grads[2], carry[3] + param_grads[3], carry[4] + gain_part, carry[5] + shift_part)
        return (updated, (merge(result[0]), merge(grad_tokens[0])))
    totals_out, (result, grad_tokens) = lax.scan(per_sample, initial, (tokens, upstream))
    return (result, grad_tokens, totals_out[0], totals_out[1], totals_out[2], totals_out[3], totals_out[4], totals_out[5])
```

```python
import functools
import math

import jax
import jax.numpy as jnp
import numpy as np
from jax import lax
from jax.experimental import pallas as pl
from jax.experimental.pallas import tpu as pltpu
from jax.sharding import Mesh
from jax.sharding import PartitionSpec as P

LAT_ROWS = 64
LON = 180
MODES = 91
CH = 96
GROUP = 32
GROUPS = CH // GROUP
SPAN = GROUP * LON
PITCH = 40
EMBED = 768
layer_eps = 1e-05
shrink = 0.1
f32 = jnp.float32
bf16 = jnp.bfloat16


def split_table(table):
    high = table.astype(np.float32).astype(bf16)
    low = (table - high.astype(np.float64)).astype(np.float32).astype(bf16)
    return high, low


@functools.cache
def tables():
    m = np.arange(33)[:, None]
    h = np.arange(LAT_ROWS)[None, :]
    ang = 2.0 * np.pi * ((m * h) % LAT_ROWS) / LAT_ROWS
    lat = np.concatenate([np.cos(ang), np.sin(ang)[1:32]], axis=0) / math.sqrt(LAT_ROWS)
    w = np.arange(LON)[:, None]
    k = np.arange(MODES)[None, :]
    ang = 2.0 * np.pi * ((w * k) % LON) / LON
    lon = np.zeros((256, 256))
    lon[:LON, :MODES] = np.cos(ang) / math.sqrt(LON)
    lon[:LON, 128 : 128 + MODES] = np.sin(ang) / math.sqrt(LON)
    lon[:LON, 128 + MODES - 1] = 0.0
    lon[:LON, 128] = 0.0
    double = np.zeros((256,))
    double[:MODES] = 2.0
    double[128 : 128 + MODES] = 2.0
    double[[0, MODES - 1, 128, 128 + MODES - 1]] = 1.0
    return lat, lon, lon * double[None, :]


def split(x):
    high = x.astype(bf16)
    return high, (x - high.astype(f32)).astype(bf16)


def dot(a, b):
    return jnp.dot(a, b, preferred_element_type=f32)


def dot_nt(a, b):
    return lax.dot_general(a, b, (((1,), (1,)), ((), ())), preferred_element_type=f32)


def to_spectrum_kernel(x_ref, lat_ref, lonh_ref, lonl_ref, re_ref, im_ref, zs, ya, yb):
    @pl.when(pl.program_id(0) == 0)
    def _():
        ya[...] = jnp.zeros_like(ya)
        yb[...] = jnp.zeros_like(yb)

    x = x_ref[...].reshape(LAT_ROWS, SPAN)
    both = dot(lat_ref[...], x)
    zs[...] = both[:LAT_ROWS] + both[LAT_ROWS:]
    for c in range(GROUP):
        v = zs[:, c * LON : (c + 1) * LON]
        ya[pl.ds(c, LAT_ROWS, stride=PITCH), :] = v[:, :128]
        yb[pl.ds(c, LAT_ROWS, stride=PITCH), 0 : LON - 128] = v[:, 128:]
    rows = jnp.concatenate([ya[...], yb[...]], axis=1)
    rows = rows.reshape(LAT_ROWS, PITCH, 256)[:, :GROUP].reshape(LAT_ROWS * GROUP, 256)
    high, low = split(rows)
    p = dot(high, lonh_ref[...]) + dot(low, lonh_ref[...]) + dot(high, lonl_ref[...])
    p = p.reshape(LAT_ROWS, GROUP, 256)
    cc, cs = p[:, :, :128], p[:, :, 128:]
    re_ref[0:1] = cc[0:1]
    im_ref[0:1] = -cs[0:1]
    re_ref[32:33] = cc[32:33]
    im_ref[32:33] = -cs[32:33]
    re_ref[1:32] = cc[1:32] - cs[33:64]
    re_ref[33:64] = cc[1:32] + cs[33:64]
    im_ref[1:32] = -cs[1:32] - cc[33:64]
    im_ref[33:64] = cc[33:64] - cs[1:32]


def to_spectrum(x, doubled):
    lat, lon, lon2 = tables()
    lat_h, lat_l = split_table(lat)
    lon_h, lon_l = split_table(lon2 if doubled else lon)
    lat_table = jnp.asarray(np.concatenate([lat_h, lat_l], axis=0))
    full = lambda *s: pl.BlockSpec(s, lambda i: (0,) * len(s))
    spec = pl.BlockSpec((LAT_ROWS, GROUP, 128), lambda i: (0, i, 0))
    shape = jax.ShapeDtypeStruct((LAT_ROWS, CH, 128), f32)
    return pl.pallas_call(
        to_spectrum_kernel,
        grid=(GROUPS,),
        in_specs=[pl.BlockSpec((32, 2, SPAN), lambda i: (0, 0, i)), full(128, 64), full(256, 256), full(256, 256)],
        out_specs=[spec, spec],
        out_shape=[shape, shape],
        scratch_shapes=[
            pltpu.VMEM((LAT_ROWS, SPAN), f32),
            pltpu.VMEM((LAT_ROWS * PITCH, 128), f32),
            pltpu.VMEM((LAT_ROWS * PITCH, 128), f32),
        ],
        cost_estimate=pl.CostEstimate(flops=8_000_000_000, bytes_accessed=9_000_000, transcendentals=0),
        compiler_params=pltpu.CompilerParams(vmem_limit_bytes=48 * 2**20),
        name="to_spectrum",
    )(x, lat_table, jnp.asarray(lon_h), jnp.asarray(lon_l))


def to_field_kernel(re_ref, im_ref, lath_ref, latl_ref, lonh_ref, lonl_ref, o_ref, zs, va, vb):
    gr, gi = re_ref[...], im_ref[...]
    left = jnp.concatenate([gr[0:1], gr[1:32] + gr[33:64], gr[32:33], gi[33:64] - gi[1:32]], axis=0)
    right = -jnp.concatenate([gi[0:1], gi[1:32] + gi[33:64], gi[32:33], gr[1:32] - gr[33:64]], axis=0)
    rows = jnp.concatenate([left, right], axis=2).reshape(LAT_ROWS * GROUP, 256).astype(bf16)
    v = dot(rows, lonh_ref[...]) + dot(rows, lonl_ref[...])
    v = v.reshape(LAT_ROWS, GROUP, 256)
    va[:, 0:GROUP, :] = v[:, :, :128]
    vb[:, 0:GROUP, :] = v[:, :, 128:]
    va2, vb2 = va.reshape(LAT_ROWS * PITCH, 128), vb.reshape(LAT_ROWS * PITCH, 128)
    for c in range(GROUP):
        zs[:, c * LON : c * LON + 128] = va2[pl.ds(c, LAT_ROWS, stride=PITCH), :]
        zs[:, c * LON + 128 : (c + 1) * LON] = vb2[pl.ds(c, LAT_ROWS, stride=PITCH), 0 : LON - 128]
    z = zs[...].astype(bf16)
    out = dot(lath_ref[...], z) + dot(latl_ref[...], z)
    o_ref[...] = out.astype(bf16).reshape(32, 2, SPAN)


def to_field(re, im, doubled):
    lat, lon, lon2 = tables()
    lat_h, lat_l = split_table(lat.T)
    lon_h, lon_l = split_table((lon2 if doubled else lon).T)
    full = lambda *s: pl.BlockSpec(s, lambda i: (0,) * len(s))
    spec = pl.BlockSpec((LAT_ROWS, GROUP, 128), lambda i: (0, i, 0))
    return pl.pallas_call(
        to_field_kernel,
        grid=(GROUPS,),
        in_specs=[spec, spec, full(64, 64), full(64, 64), full(256, 256), full(256, 256)],
        out_specs=pl.BlockSpec((32, 2, SPAN), lambda i: (0, 0, i)),
        out_shape=jax.ShapeDtypeStruct((32, 2, CH * LON), bf16),
        scratch_shapes=[
            pltpu.VMEM((LAT_ROWS, SPAN), f32),
            pltpu.VMEM((LAT_ROWS, PITCH, 128), f32),
            pltpu.VMEM((LAT_ROWS, PITCH, 128), f32),
        ],
        cost_estimate=pl.CostEstimate(flops=8_000_000_000, bytes_accessed=9_000_000, transcendentals=0),
        compiler_params=pltpu.CompilerParams(vmem_limit_bytes=48 * 2**20),
        name="to_field",
    )(re, im, jnp.asarray(lat_h), jnp.asarray(lat_l), jnp.asarray(lon_h), jnp.asarray(lon_l))


STEP = 8


def gather_modes(re, im):
    return jnp.concatenate([jnp.concatenate([re[j], im[j]], axis=0) for j in range(STEP)], axis=1)


def mlp_forward_kernel(
    re_ref, im_ref, w1_ref, b1_ref, w2_ref, b2_ref, ore_ref, oim_ref, s_ref, g_ref, h_ref, t_ref,
    w1h, w1l, w2h, w2l,
):
    @pl.when(pl.program_id(0) == 0)
    def _():
        w1h[...], w1l[...] = split(w1_ref[...])
        w2h[...], w2l[...] = split(w2_ref[...])

    x = gather_modes(re_ref[...], im_ref[...])
    xh, xl = split(x)
    pre = dot(w1h[...], xh) + dot(w1h[...], xl) + dot(w1l[...], xh) + b1_ref[...]
    a = math.sqrt(2.0 / math.pi)
    sq = pre * pre
    th = jnp.tanh(a * pre * (1.0 + 0.044715 * sq))
    half = 0.5 * (1.0 + th)
    hid = pre * half
    slope = half + 0.5 * pre * (1.0 - th * th) * (a * (1.0 + 3.0 * 0.044715 * sq))
    hh, hl = split(hid)
    pre2 = dot(w2h[...], hh) + dot(w2h[...], hl) + dot(w2l[...], hh) + b2_ref[...]
    t = jnp.tanh(pre2 * (1.0 / shrink))
    mixed = pre2 - shrink * t
    for j in range(STEP):
        ore_ref[j] = mixed[:CH, 128 * j : 128 * (j + 1)]
        oim_ref[j] = mixed[CH:, 128 * j : 128 * (j + 1)]
    s_ref[0] = xh
    g_ref[0] = slope.astype(bf16)
    h_ref[0] = hh
    t_ref[0] = (t * t).astype(bf16)


def mlp_forward(re, im, mats, bias):
    w1, w2 = mats
    b1, b2 = bias
    n = LAT_ROWS // STEP
    full = lambda *s: pl.BlockSpec(s, lambda i: (0,) * len(s))
    spec = pl.BlockSpec((STEP, CH, 128), lambda i: (i, 0, 0))
    shape = jax.ShapeDtypeStruct((LAT_ROWS, CH, 128), f32)
    sspec = pl.BlockSpec((1, 2 * CH, 128 * STEP), lambda i: (i, 0, 0))
    sshape = jax.ShapeDtypeStruct((n, 2 * CH, 128 * STEP), bf16)
    mat, vec = full(192, 192), full(192, 1)
    return pl.pallas_call(
        mlp_forward_kernel,
        grid=(n,),
        in_specs=[spec, spec, mat, vec, mat, vec],
        out_specs=[spec, spec] + [sspec] * 4,
        out_shape=[shape, shape] + [sshape] * 4,
        scratch_shapes=[pltpu.VMEM((192, 192), bf16)] * 4,
        cost_estimate=pl.CostEstimate(flops=8_000_000_000, bytes_accessed=24_000_000, transcendentals=0),
        compiler_params=pltpu.CompilerParams(vmem_limit_bytes=48 * 2**20),
        name="mlp_forward",
    )(re, im, w1, b1, w2, b2)


def mlp_backward_kernel(
    re_ref, im_ref, s_ref, g_ref, h_ref, t_ref, w1_ref, w2_ref,
    ore_ref, oim_ref, d1_ref, e1_ref, d2_ref, e2_ref, a1, a2, c1, c2,
):
    step = pl.program_id(0)

    @pl.when(step == 0)
    def _():
        for r in (a1, a2, c1, c2):
            r[...] = jnp.zeros_like(r)

    p2 = gather_modes(re_ref[...], im_ref[...]) * t_ref[0].astype(f32)
    p2h = p2.astype(bf16)
    p1 = dot(w2_ref[...], p2h) * g_ref[0].astype(f32)
    p1h = p1.astype(bf16)
    out = dot(w1_ref[...], p1h)
    for j in range(STEP):
        ore_ref[j] = out[:CH, 128 * j : 128 * (j + 1)]
        oim_ref[j] = out[CH:, 128 * j : 128 * (j + 1)]
    a2[...] += dot_nt(h_ref[0], p2h)
    a1[...] += dot_nt(s_ref[0], p1h)
    c2[...] += sum(p2[:, 128 * j : 128 * (j + 1)] for j in range(STEP))
    c1[...] += sum(p1[:, 128 * j : 128 * (j + 1)] for j in range(STEP))

    @pl.when(step == pl.num_programs(0) - 1)
    def _():
        for acc, out_ref in ((a1, d1_ref), (a2, d2_ref)):
            v = acc[...]
            out_ref[0] = v[:CH, :CH] + v[CH:, CH:]
            out_ref[1] = v[:CH, CH:] - v[CH:, :CH]
        for acc, out_ref in ((c1, e1_ref), (c2, e2_ref)):
            out_ref[...] = jnp.sum(acc[...], axis=1, keepdims=True)


def mlp_backward(re, im, stash, w1, w2):
    n = LAT_ROWS // STEP
    full = lambda *s: pl.BlockSpec(s, lambda i: (0,) * len(s))
    spec = pl.BlockSpec((STEP, CH, 128), lambda i: (i, 0, 0))
    shape = jax.ShapeDtypeStruct((LAT_ROWS, CH, 128), f32)
    sspec = pl.BlockSpec((1, 2 * CH, 128 * STEP), lambda i: (i, 0, 0))
    mat = full(192, 192)
    d, e = jax.ShapeDtypeStruct((2, CH, CH), f32), jax.ShapeDtypeStruct((192, 1), f32)
    return pl.pallas_call(
        mlp_backward_kernel,
        grid=(n,),
        in_specs=[spec, spec] + [sspec] * 4 + [mat, mat],
        out_specs=[spec, spec, full(2, CH, CH), full(192, 1), full(2, CH, CH), full(192, 1)],
        out_shape=[shape, shape, d, e, d, e],
        scratch_shapes=[pltpu.VMEM((192, 192), f32)] * 2 + [pltpu.VMEM((192, 128), f32)] * 2,
        cost_estimate=pl.CostEstimate(flops=8_000_000_000, bytes_accessed=24_000_000, transcendentals=0),
        compiler_params=pltpu.CompilerParams(vmem_limit_bytes=48 * 2**20),
        name="mlp_backward",
    )(re, im, *stash, w1, w2)


def big_matrix(weight):
    real, imag = weight[0, 0], weight[1, 0]
    return jnp.block([[real, imag], [-imag, real]])


def lane_parts(ref_or_value):
    return [slice(c * LON, (c + 1) * LON) for c in range(GROUP)]


def widen(dst, values):
    for part in lane_parts(dst):
        dst[:, part] = values


def narrow(src):
    total = None
    for part in lane_parts(src):
        v = src[:, part]
        total = v if total is None else total + v
    return total


def load_rows(ref):
    return ref[...].reshape(LAT_ROWS, SPAN).astype(f32)


def norm_sums_kernel(x_ref, o_ref, first, second):
    step = pl.program_id(0)

    @pl.when(step == 0)
    def _():
        first[...] = jnp.zeros_like(first)
        second[...] = jnp.zeros_like(second)

    x = load_rows(x_ref)
    first[...] += x
    second[...] += x * x

    @pl.when(step == pl.num_programs(0) - 1)
    def _():
        o_ref[:, 0:LON] = narrow(first)
        o_ref[:, LON : 2 * LON] = narrow(second)
        o_ref[:, 2 * LON :] = jnp.zeros((LAT_ROWS, 384 - 2 * LON), f32)


def prepare_norm(sums_ref, center, scale):
    sums = sums_ref[0]
    for p in range(1, sums_ref.shape[0]):
        sums = sums + sums_ref[p]
    mean = sums[:, 0:LON] * (1.0 / EMBED)
    variance = sums[:, LON : 2 * LON] * (1.0 / EMBED) - mean * mean
    widen(center, mean)
    widen(scale, lax.rsqrt(variance + layer_eps))


def normalize_kernel(x_ref, sums_ref, gain_ref, shift_ref, o_ref, center, scale):
    @pl.when(pl.program_id(0) == 0)
    def _():
        prepare_norm(sums_ref, center, scale)

    standard = (load_rows(x_ref) - center[...]) * scale[...]
    o_ref[...] = (standard * gain_ref[...] + shift_ref[...]).astype(bf16).reshape(32, 2, SPAN)


def result_kernel(x_ref, n_ref, f_ref, o_ref):
    total = x_ref[...].astype(f32) + n_ref[...].astype(f32) + f_ref[...].astype(f32)
    o_ref[...] = total.astype(bf16)


def result_rows_kernel(x_ref, n_ref, f_ref, o_ref):
    total = load_rows(x_ref) + load_rows(n_ref) + load_rows(f_ref)
    o_ref[...] = total.astype(bf16).reshape(32, 2, SPAN)


def grad_sums_kernel(
    x_ref, u_ref, s_ref, sums_ref, gain_ref, o_ref, part_ref, center, scale, first, second
):
    step = pl.program_id(0)

    @pl.when(step == 0)
    def _():
        prepare_norm(sums_ref, center, scale)
        first[...] = jnp.zeros_like(first)
        second[...] = jnp.zeros_like(second)

    standard = (load_rows(x_ref) - center[...]) * scale[...]
    grad = load_rows(u_ref) + load_rows(s_ref)
    cross = grad * standard
    gain = gain_ref[...]
    first[...] += grad * gain
    second[...] += cross * gain
    part_ref[0:1, :] = jnp.sum(cross, axis=0, keepdims=True)
    part_ref[1:2, :] = jnp.sum(grad, axis=0, keepdims=True)

    @pl.when(step == pl.num_programs(0) - 1)
    def _():
        o_ref[:, 0:LON] = narrow(first)
        o_ref[:, LON : 2 * LON] = narrow(second)
        o_ref[:, 2 * LON :] = jnp.zeros((LAT_ROWS, 384 - 2 * LON), f32)


def grad_tokens_kernel(
    x_ref, u_ref, s_ref, sums_ref, grads_ref, gain_ref, o_ref, center, scale, mean_grad, cross_grad
):
    @pl.when(pl.program_id(0) == 0)
    def _():
        prepare_norm(sums_ref, center, scale)
        sums = grads_ref[0]
        for p in range(1, grads_ref.shape[0]):
            sums = sums + grads_ref[p]
        widen(mean_grad, sums[:, 0:LON] * (1.0 / EMBED))
        widen(cross_grad, sums[:, LON : 2 * LON] * (1.0 / EMBED))

    inverse = scale[...]
    standard = (load_rows(x_ref) - center[...]) * inverse
    up = load_rows(u_ref)
    grad = (up + load_rows(s_ref)) * gain_ref[...]
    out = up + inverse * (grad - mean_grad[...] - standard * cross_grad[...])
    o_ref[...] = out.astype(bf16).reshape(32, 2, SPAN)


def row_call(kernel, name, ins, outs, scratch):
    field = pl.BlockSpec((32, 2, SPAN), lambda i: (0, 0, i))
    line = lambda rows: pl.BlockSpec((rows, SPAN), lambda i: (0, i))

    def spec(x):
        if x.shape == (32, 2, CH * LON):
            return field
        if x.ndim == 2 and x.shape[1] == CH * LON:
            return line(x.shape[0])
        return pl.BlockSpec(x.shape, lambda i: (0,) * x.ndim)

    many = len(outs) > 1
    return pl.pallas_call(
        kernel,
        grid=(GROUPS,),
        in_specs=[spec(x) for x in ins],
        out_specs=[spec(x) for x in outs] if many else spec(outs[0]),
        out_shape=list(outs) if many else outs[0],
        scratch_shapes=[pltpu.VMEM((LAT_ROWS, SPAN), f32)] * scratch,
        cost_estimate=pl.CostEstimate(flops=3_000_000_000, bytes_accessed=8_000_000, transcendentals=0),
        compiler_params=pltpu.CompilerParams(vmem_limit_bytes=48 * 2**20),
        name=name,
    )(*ins)


FIELD = jax.ShapeDtypeStruct((32, 2, CH * LON), bf16)
SUMS = jax.ShapeDtypeStruct((LAT_ROWS, 384), f32)


def exchange(x, axes):
    return lax.all_to_all(x, axes, 0, 0, tiled=True)


def from_everyone(x, axes):
    peers = lax.axis_size(axes)
    return exchange(jnp.broadcast_to(x[None], (peers, *x.shape)), axes)


def reduced(line, axes):
    peers = lax.axis_size(axes)
    size = -(-line.size // (peers * 128)) * 128
    line = jnp.pad(line, (0, peers * size - line.size))
    mine = exchange(line.reshape(peers, 1, size), axes).sum(axis=0)
    return lax.all_gather(mine, axes, axis=0, tiled=True).reshape(-1)


def body(
    tokens, norm_gain, norm_shift, first_weight, first_bias, second_weight, second_bias, upstream
):
    lat = ("lat",)
    wide = lambda v: jnp.broadcast_to(v[:, None], (CH, LON)).reshape(1, CH * LON)
    gain, shift = wide(norm_gain), wide(norm_shift)
    first, second = big_matrix(first_weight), big_matrix(second_weight)
    bias = (first_bias.reshape(2 * CH, 1), second_bias.reshape(2 * CH, 1))

    upstream_columns = exchange(upstream, lat)
    sums = from_everyone(row_call(norm_sums_kernel, "norm_sums", (tokens,), (SUMS,), 2), "ch")
    normed = row_call(normalize_kernel, "normalize", (tokens, sums, gain, shift), (FIELD,), 2)
    normed_columns = exchange(normed, lat)
    up_re, up_im = to_spectrum(upstream_columns, True)
    re, im = to_spectrum(normed_columns, False)
    re, im, *stash = mlp_forward(re, im, (first.T, second.T), bias)
    filtered = exchange(to_field(re, im, True), lat)
    re, im, d1, e1, d2, e2 = mlp_backward(
        up_re, up_im, stash, first.astype(bf16), second.astype(bf16)
    )
    spectral = exchange(to_field(re, im, False), lat)
    result = row_call(result_kernel, "result", (tokens, normed, filtered), (FIELD,), 0)
    line = reduced(jnp.concatenate([a.reshape(-1) for a in (d1, d2, e1, e2)]), lat)
    n = 2 * CH * CH
    gfw, gsw = line[:n].reshape(2, 1, CH, CH), line[n : 2 * n].reshape(2, 1, CH, CH)
    gfb = line[2 * n : 2 * n + 192].reshape(2, 1, CH)
    gsb = line[2 * n + 192 : 2 * n + 384].reshape(2, 1, CH)
    sums2, parts = row_call(
        grad_sums_kernel, "grad_sums", (tokens, upstream, spectral, sums, gain),
        (SUMS, jax.ShapeDtypeStruct((2, CH * LON), f32)), 4,
    )
    sums2 = from_everyone(sums2, "ch")
    grad_tokens = row_call(
        grad_tokens_kernel, "grad_tokens", (tokens, upstream, spectral, sums, sums2, gain), (FIELD,), 4
    )
    ends = jnp.sum(parts.reshape(2 * CH, LON), axis=1)
    ends = from_everyone(ends[None], lat).sum(axis=(0, 1))
    return result, grad_tokens, gfw, gfb, gsw, gsb, ends[:CH], ends[CH:]


def solution(mesh):
    whole, weight, bias = P(None, "lat", "ch"), P(None, "ch", None, None), P(None, "ch", None)
    return jax.shard_map(
        body,
        mesh=mesh,
        in_specs=(whole, P("ch"), P("ch"), weight, bias, weight, bias, whole),
        out_specs=(whole, whole, weight, bias, weight, bias, P("ch"), P("ch")),
        check_vma=False,
    )
```

```python
import functools
import math

import jax
import jax.numpy as jnp
import numpy as np
from jax import lax
from jax.experimental import pallas as pl
from jax.experimental.pallas import tpu as pltpu
from jax.sharding import Mesh
from jax.sharding import PartitionSpec as P

LAT_ROWS = 64
LON = 180
MODES = 91
CH = 96
GROUP = 32
GROUPS = CH // GROUP
SPAN = GROUP * LON
PITCH = 40
EMBED = 768
layer_eps = 1e-05
shrink = 0.1
f32 = jnp.float32
bf16 = jnp.bfloat16


def split_table(table):
    high = table.astype(np.float32).astype(bf16)
    low = (table - high.astype(np.float64)).astype(np.float32).astype(bf16)
    return high, low


@functools.cache
def tables():
    m = np.arange(33)[:, None]
    h = np.arange(LAT_ROWS)[None, :]
    ang = 2.0 * np.pi * ((m * h) % LAT_ROWS) / LAT_ROWS
    lat = np.concatenate([np.cos(ang), np.sin(ang)[1:32]], axis=0) / math.sqrt(LAT_ROWS)
    w = np.arange(LON)[:, None]
    k = np.arange(MODES)[None, :]
    ang = 2.0 * np.pi * ((w * k) % LON) / LON
    lon = np.zeros((256, 256))
    lon[:LON, :MODES] = np.cos(ang) / math.sqrt(LON)
    lon[:LON, 128 : 128 + MODES] = np.sin(ang) / math.sqrt(LON)
    lon[:LON, 128 + MODES - 1] = 0.0
    lon[:LON, 128] = 0.0
    double = np.zeros((256,))
    double[:MODES] = 2.0
    double[128 : 128 + MODES] = 2.0
    double[[0, MODES - 1, 128, 128 + MODES - 1]] = 1.0
    return lat, lon, lon * double[None, :]


def split(x):
    high = x.astype(bf16)
    return high, (x - high.astype(f32)).astype(bf16)


def dot(a, b):
    return jnp.dot(a, b, preferred_element_type=f32)


def dot_nt(a, b):
    return lax.dot_general(a, b, (((1,), (1,)), ((), ())), preferred_element_type=f32)


STEP = 8


def gather_modes(re, im):
    return jnp.concatenate([jnp.concatenate([re[j], im[j]], axis=0) for j in range(STEP)], axis=1)


def big_matrix(weight):
    real, imag = weight[0, 0], weight[1, 0]
    return jnp.block([[real, imag], [-imag, real]])


def lane_parts(ref_or_value):
    return [slice(c * LON, (c + 1) * LON) for c in range(GROUP)]


def widen(dst, values):
    for part in lane_parts(dst):
        dst[:, part] = values


def narrow(src):
    total = None
    for part in lane_parts(src):
        v = src[:, part]
        total = v if total is None else total + v
    return total


MESH = pl.DeviceIdType.MESH
UP, NORM, FILT, GRAD = range(4)


def mega_kernel(
    tokens, upstream, gain_ref, shift_ref, w1_ref, b1_ref, w2_ref, b2_ref,
    lat_ref, lonh, lonl, latih, latil, lonih, lonil,
    result, grad_tokens, params_out, ends_out,
    tok, upr, cols, normed, filt, grad, spec, stash, zs, ya, yb, center, scale, first, second,
    sums_send, sums_recv, wh, wl, wt, a1, a2, c1, c2, pack, packed_recv, piece, parts, ends_send, ends_recv,
    load_sem, store_sem, send_sem, recv_sem, ch_send, ch_recv, small_send, small_recv,
):
    lat = lax.axis_index("lat")
    ch = lax.axis_index("ch")
    peers, chs = 32, 8

    def peer_at(s):
        return lax.rem(lat + 64 + ((s + 1) // 2) * (2 * lax.rem(s, 2) - 1), peers)

    def lanes(g):
        return pl.ds(pl.multiple_of(g * SPAN, SPAN), SPAN)

    def each_peer(fn):
        lax.fori_loop(1, peers, lambda s, z: (fn(peer_at(s)), z)[1], 0)

    def each_ch(fn):
        lax.fori_loop(1, chs, lambda s, z: (fn(lax.rem(ch + s, chs)), z)[1], 0)

    loads = [
        pltpu.make_async_copy(upstream, upr, load_sem.at[0]),
        pltpu.make_async_copy(tokens, tok, load_sem.at[1]),
    ]
    for c in loads:
        c.start()

    barrier = pltpu.get_barrier_semaphore()
    each_peer(lambda p: pl.semaphore_signal(barrier, inc=1, device_id={"lat": p}, device_id_type=MESH))
    each_ch(lambda p: pl.semaphore_signal(barrier, inc=1, device_id={"ch": p}, device_id_type=MESH))
    pl.semaphore_wait(barrier, peers - 1 + chs - 1)

    def send_field(src, dst, kind, g):
        def go(p):
            pltpu.make_async_remote_copy(
                src_ref=src.at[p, :, lanes(g)],
                dst_ref=dst.at[lat, :, lanes(g)],
                send_sem=send_sem.at[kind, g],
                recv_sem=recv_sem.at[kind, g],
                device_id={"lat": p},
                device_id_type=MESH,
            ).start()

        each_peer(go)

    def wait_bytes(buf, sem):
        ref = buf.at[pl.ds(0, peers - 1)]
        pltpu.make_async_copy(ref, ref, sem).wait()

    def wait_field(buf, sem, kind, g):
        ref = buf.at[pl.ds(0, peers - 1), :, lanes(g)]
        pltpu.make_async_copy(ref, ref, sem.at[kind, g]).wait()

    def keep_own(src, dst, g):
        dst[lat, :, lanes(g)] = src[lat, :, lanes(g)]

    loads[0].wait()
    send_field(upr, cols.at[0], UP, 0)
    send_field(upr, cols.at[0], UP, 1)
    loads[1].wait()

    def rows_of(ref, g):
        return ref[:, :, lanes(g)].reshape(LAT_ROWS, SPAN).astype(f32)

    def put_rows(ref, g, value):
        ref[:, :, lanes(g)] = value.astype(bf16).reshape(32, 2, SPAN)

    def over_channels(which):
        sums_send[which, :, 0:LON] = narrow(first)
        sums_send[which, :, LON : 2 * LON] = narrow(second)
        sums_send[which, :, 2 * LON :] = jnp.zeros((LAT_ROWS, 384 - 2 * LON), f32)
        sums_recv[which, ch] = sums_send[which]

        def go(p):
            pltpu.make_async_remote_copy(
                src_ref=sums_send.at[which],
                dst_ref=sums_recv.at[which, ch],
                send_sem=ch_send.at[which],
                recv_sem=ch_recv.at[which],
                device_id={"ch": p},
                device_id_type=MESH,
            ).start()

        each_ch(go)

    def wait_channels(which):
        ref = sums_recv.at[which, pl.ds(0, chs - 1)]
        pltpu.make_async_copy(ref, ref, ch_recv.at[which]).wait()
        total = sums_recv[which, 0]
        for p in range(1, chs):
            total = total + sums_recv[which, p]
        return total * (1.0 / EMBED)

    first[...] = jnp.zeros_like(first)
    second[...] = jnp.zeros_like(second)

    @pl.loop(0, GROUPS)
    def _(g):
        x = rows_of(tok, g)
        first[...] += x
        second[...] += x * x

    over_channels(0)
    ya[...] = jnp.zeros_like(ya)
    yb[...] = jnp.zeros_like(yb)
    wh[0], wl[0] = split(w1_ref[...].T)
    wh[1], wl[1] = split(w2_ref[...].T)
    wt[0] = w1_ref[...].astype(bf16)
    wt[1] = w2_ref[...].astype(bf16)
    for g in range(GROUPS):
        keep_own(upr, cols.at[0], g)
    for r in (a1, a2, c1, c2):
        r[...] = jnp.zeros_like(r)
    sums = wait_channels(0)
    mean = sums[:, 0:LON]
    variance = sums[:, LON : 2 * LON] - mean * mean
    widen(center, mean)
    widen(scale, lax.rsqrt(variance + layer_eps))

    @pl.loop(0, GROUPS)
    def _(g):
        standard = (rows_of(tok, g) - center[...]) * scale[...]
        put_rows(normed, g, standard * gain_ref[:, lanes(g)] + shift_ref[:, lanes(g)])
        keep_own(normed, cols.at[1], g)
        send_field(normed, cols.at[1], NORM, g)

    send_field(upr, cols.at[0], UP, 2)

    def spectrum(field, g):
        x = cols[field, :, :, lanes(g)].reshape(LAT_ROWS, SPAN)
        both = dot(lat_ref[...], x)
        zs[...] = both[:LAT_ROWS] + both[LAT_ROWS:]
        for c in range(GROUP):
            v = zs[:, c * LON : (c + 1) * LON]
            ya[pl.ds(c, LAT_ROWS, stride=PITCH), :] = v[:, :128]
            yb[pl.ds(c, LAT_ROWS, stride=PITCH), 0 : LON - 128] = v[:, 128:]
        rows = jnp.concatenate([ya[...], yb[...]], axis=1)
        rows = rows.reshape(LAT_ROWS, PITCH, 256)[:, :GROUP].reshape(LAT_ROWS * GROUP, 256)
        high, low = split(rows)
        p = dot(high, lonh[field]) + dot(low, lonh[field]) + dot(high, lonl[field])
        p = p.reshape(LAT_ROWS, GROUP, 256)
        cc, cs = p[:, :, :128], p[:, :, 128:]
        here = pl.ds(pl.multiple_of(g * GROUP, GROUP), GROUP)
        re, im = spec.at[field, 0], spec.at[field, 1]
        re[0:1, here] = cc[0:1]
        im[0:1, here] = -cs[0:1]
        re[32:33, here] = cc[32:33]
        im[32:33, here] = -cs[32:33]
        re[1:32, here] = cc[1:32] - cs[33:64]
        re[33:64, here] = cc[1:32] + cs[33:64]
        im[1:32, here] = -cs[1:32] - cc[33:64]
        im[33:64, here] = cc[33:64] - cs[1:32]

    @pl.loop(0, 2)
    def _(g):
        wait_field(cols.at[0], recv_sem, UP, g)
        spectrum(0, g)

    @pl.loop(0, GROUPS)
    def _(g):
        wait_field(cols.at[1], recv_sem, NORM, g)
        spectrum(1, g)

    @pl.loop(0, LAT_ROWS // STEP)
    def _(i):
        at = pl.ds(i * STEP, STEP)
        re, im = spec.at[1, 0], spec.at[1, 1]
        xh, xl = split(gather_modes(re[at], im[at]))
        pre = dot(wh[0], xh) + dot(wh[0], xl) + dot(wl[0], xh) + b1_ref[...]
        a = math.sqrt(2.0 / math.pi)
        sq = pre * pre
        th = jnp.tanh(a * pre * (1.0 + 0.044715 * sq))
        half = 0.5 * (1.0 + th)
        hid = pre * half
        slope = half + 0.5 * pre * (1.0 - th * th) * (a * (1.0 + 3.0 * 0.044715 * sq))
        hh, hl = split(hid)
        pre2 = dot(wh[1], hh) + dot(wh[1], hl) + dot(wl[1], hh) + b2_ref[...]
        t = jnp.tanh(pre2 * (1.0 / shrink))
        mixed = pre2 - shrink * t
        for j in range(STEP):
            re[i * STEP + j] = mixed[:CH, 128 * j : 128 * (j + 1)]
            im[i * STEP + j] = mixed[CH:, 128 * j : 128 * (j + 1)]
        stash[0, i] = xh
        stash[1, i] = slope.astype(bf16)
        stash[2, i] = hh
        stash[3, i] = (t * t).astype(bf16)

    def field_of(field, g, dst):
        here = pl.ds(pl.multiple_of(g * GROUP, GROUP), GROUP)
        gr, gi = spec[field, 0, :, here], spec[field, 1, :, here]
        left = jnp.concatenate([gr[0:1], gr[1:32] + gr[33:64], gr[32:33], gi[33:64] - gi[1:32]], axis=0)
        right = -jnp.concatenate([gi[0:1], gi[1:32] + gi[33:64], gi[32:33], gr[1:32] - gr[33:64]], axis=0)
        rows = jnp.concatenate([left, right], axis=2).reshape(LAT_ROWS * GROUP, 256).astype(bf16)
        v = dot(rows, lonih[field]) + dot(rows, lonil[field])
        v = v.reshape(LAT_ROWS, GROUP, 256)
        va, vb = ya.reshape(LAT_ROWS, PITCH, 128), yb.reshape(LAT_ROWS, PITCH, 128)
        va[:, 0:GROUP, :] = v[:, :, :128]
        vb[:, 0:GROUP, :] = v[:, :, 128:]
        for c in range(GROUP):
            zs[:, c * LON : c * LON + 128] = ya[pl.ds(c, LAT_ROWS, stride=PITCH), :]
            zs[:, c * LON + 128 : (c + 1) * LON] = yb[pl.ds(c, LAT_ROWS, stride=PITCH), 0 : LON - 128]
        z = zs[...].astype(bf16)
        put_rows(dst, g, dot(latih[...], z) + dot(latil[...], z))

    @pl.loop(0, GROUPS)
    def _(g):
        field_of(1, g, cols.at[1])
        keep_own(cols.at[1], filt, g)
        send_field(cols.at[1], filt, FILT, g)

    wait_field(cols.at[0], recv_sem, UP, 2)
    yb[:, LON - 128 :] = jnp.zeros((LAT_ROWS * PITCH, 256 - LON), f32)
    spectrum(0, 2)

    @pl.loop(0, LAT_ROWS // STEP)
    def _(i):
        at = pl.ds(i * STEP, STEP)
        re, im = spec.at[0, 0], spec.at[0, 1]
        p2 = gather_modes(re[at], im[at]) * stash[3, i].astype(f32)
        p2h = p2.astype(bf16)
        p1 = dot(wt[1], p2h) * stash[1, i].astype(f32)
        p1h = p1.astype(bf16)
        out = dot(wt[0], p1h)
        for j in range(STEP):
            re[i * STEP + j] = out[:CH, 128 * j : 128 * (j + 1)]
            im[i * STEP + j] = out[CH:, 128 * j : 128 * (j + 1)]
        a2[...] += dot_nt(stash[2, i], p2h)
        a1[...] += dot_nt(stash[0, i], p1h)
        c2[...] += sum(p2[:, 128 * j : 128 * (j + 1)] for j in range(STEP))
        c1[...] += sum(p1[:, 128 * j : 128 * (j + 1)] for j in range(STEP))

    @pl.loop(0, GROUPS)
    def _(g):
        field_of(0, g, cols.at[0])
        keep_own(cols.at[0], grad, g)
        send_field(cols.at[0], grad, GRAD, g)

    pack[...] = jnp.zeros_like(pack)
    for n, (acc, line) in enumerate(((a1, c1), (a2, c2))):
        v = acc[...]
        top = n * 2 * CH
        pack[top : top + CH, :CH] = v[:CH, :CH] + v[CH:, CH:]
        pack[top + CH : top + 2 * CH, :CH] = v[:CH, CH:] - v[CH:, :CH]
        pack[top : top + 2 * CH, CH : CH + 1] = jnp.sum(line[...], axis=1, keepdims=True)

    def rows16(p):
        return pl.ds(pl.multiple_of(p * 16, 16), 16)

    packed_recv[lat] = pack[rows16(lat), :]

    def send_piece(p):
        pltpu.make_async_remote_copy(
            src_ref=pack.at[rows16(p), :],
            dst_ref=packed_recv.at[lat],
            send_sem=small_send.at[0],
            recv_sem=small_recv.at[0],
            device_id={"lat": p},
            device_id_type=MESH,
        ).start()

    each_peer(send_piece)

    @pl.loop(0, GROUPS)
    def _(g):
        wait_field(filt, recv_sem, FILT, g)
        put_rows(filt, g, rows_of(tok, g) + rows_of(normed, g) + rows_of(filt, g))
        pltpu.make_async_copy(filt.at[:, :, lanes(g)], result.at[:, :, lanes(g)], store_sem.at[0, g]).start()

    wait_bytes(packed_recv, small_recv.at[0])
    piece[...] = jnp.sum(packed_recv[...], axis=0)
    params_out[lat] = piece[...]

    def send_sum(p):
        pltpu.make_async_remote_copy(
            src_ref=piece,
            dst_ref=params_out.at[lat],
            send_sem=small_send.at[1],
            recv_sem=small_recv.at[1],
            device_id={"lat": p},
            device_id_type=MESH,
        ).start()

    each_peer(send_sum)

    parts[...] = jnp.zeros_like(parts)
    first[...] = jnp.zeros_like(first)
    second[...] = jnp.zeros_like(second)

    @pl.loop(0, GROUPS)
    def _(g):
        wait_field(grad, recv_sem, GRAD, g)
        standard = (rows_of(tok, g) - center[...]) * scale[...]
        total = rows_of(upr, g) + rows_of(grad, g)
        cross = total * standard
        gain = gain_ref[:, lanes(g)]
        first[...] += total * gain
        second[...] += cross * gain
        parts[0:1, lanes(g)] = jnp.sum(cross, axis=0, keepdims=True)
        parts[1:2, lanes(g)] = jnp.sum(total, axis=0, keepdims=True)

    over_channels(1)

    @pl.loop(0, GROUPS)
    def _(g):
        base = parts[:, lanes(g)]
        column = jnp.concatenate(
            [jnp.sum(base[:, c * LON : (c + 1) * LON], axis=1, keepdims=True) for c in range(GROUP)], axis=1
        )
        ends_send[g] = jnp.concatenate([column, jnp.zeros((8, 128 - GROUP), f32)], axis=1)

    ends_recv[lat] = ends_send[...]

    def send_ends(p):
        pltpu.make_async_remote_copy(
            src_ref=ends_send,
            dst_ref=ends_recv.at[lat],
            send_sem=small_send.at[2],
            recv_sem=small_recv.at[2],
            device_id={"lat": p},
            device_id_type=MESH,
        ).start()

    each_peer(send_ends)
    sums = wait_channels(1)
    widen(first, sums[:, 0:LON])
    widen(second, sums[:, LON : 2 * LON])

    @pl.loop(0, GROUPS)
    def _(g):
        inverse = scale[...]
        standard = (rows_of(tok, g) - center[...]) * inverse
        up = rows_of(upr, g)
        slope = (up + rows_of(grad, g)) * gain_ref[:, lanes(g)]
        put_rows(grad, g, up + inverse * (slope - first[...] - standard * second[...]))
        pltpu.make_async_copy(grad.at[:, :, lanes(g)], grad_tokens.at[:, :, lanes(g)], store_sem.at[1, g]).start()

    wait_bytes(ends_recv, small_recv.at[2])
    ends_out[...] = jnp.sum(ends_recv[...], axis=0)
    wait_bytes(params_out, small_recv.at[1])
    for which, buf, out in ((0, filt, result), (1, grad, grad_tokens)):
        for g in range(GROUPS):
            pltpu.make_async_copy(buf.at[:, :, lanes(g)], out.at[:, :, lanes(g)], store_sem.at[which, g]).wait()
    for kind, buf in ((UP, upr), (NORM, normed), (FILT, cols.at[1]), (GRAD, cols.at[0])):
        for g in range(GROUPS):
            wait_field(buf, send_sem, kind, g)
    for which in range(2):
        ref = sums_recv.at[which, pl.ds(0, chs - 1)]
        pltpu.make_async_copy(ref, ref, ch_send.at[which]).wait()
    wait_bytes(packed_recv, small_send.at[0])
    wait_bytes(params_out, small_send.at[1])
    wait_bytes(ends_recv, small_send.at[2])


def mega(tokens, upstream, gain, shift, w1, b1, w2, b2):
    lat, lon, lon2 = tables()
    pair = lambda a, b: [jnp.asarray(np.stack(x)) for x in zip(split_table(a), split_table(b))]
    lat_h, lat_l = split_table(lat)
    lati_h, lati_l = split_table(lat.T)
    lonh, lonl = pair(lon2, lon)
    lonih, lonil = pair(lon.T, lon2.T)
    hbm, vmem = pl.BlockSpec(memory_space=pl.ANY), pl.BlockSpec(memory_space=pltpu.VMEM)
    field = jax.ShapeDtypeStruct((32, 2, CH * LON), bf16)
    V, D = pltpu.VMEM, pltpu.SemaphoreType.DMA
    fld = V((32, 2, CH * LON), bf16)
    wide = V((LAT_ROWS, SPAN), f32)
    ins = [
        tokens, upstream, gain, shift, w1, b1, w2, b2,
        jnp.asarray(np.concatenate([lat_h, lat_l], axis=0)), lonh, lonl,
        jnp.asarray(lati_h), jnp.asarray(lati_l), lonih, lonil,
    ]
    return pl.pallas_call(
        mega_kernel,
        in_specs=[hbm, hbm] + [vmem] * (len(ins) - 2),
        out_specs=[hbm, hbm, vmem, vmem],
        out_shape=[
            field, field,
            jax.ShapeDtypeStruct((32, 16, 128), f32),
            jax.ShapeDtypeStruct((GROUPS, 8, 128), f32),
        ],
        scratch_shapes=[
            fld, fld, V((2, 32, 2, CH * LON), bf16), fld, fld, fld,
            V((2, 2, LAT_ROWS, CH, 128), f32),
            V((4, LAT_ROWS // STEP, 2 * CH, 128 * STEP), bf16),
            wide, V((LAT_ROWS * PITCH, 128), f32), V((LAT_ROWS * PITCH, 128), f32),
            wide, wide, wide, wide,
            V((2, LAT_ROWS, 384), f32), V((2, 8, LAT_ROWS, 384), f32),
            V((2, 192, 192), bf16), V((2, 192, 192), bf16), V((2, 192, 192), bf16),
            V((192, 192), f32), V((192, 192), f32), V((192, 128), f32), V((192, 128), f32),
            V((512, 128), f32), V((32, 16, 128), f32), V((16, 128), f32),
            V((8, CH * LON), f32), V((GROUPS, 8, 128), f32), V((32, GROUPS, 8, 128), f32),
            D((2,)), D((2, GROUPS)), D((4, GROUPS)), D((4, GROUPS)), D((2,)), D((2,)), D((3,)), D((3,)),
        ],
        compiler_params=pltpu.CompilerParams(
            collective_id=0, has_side_effects=True, vmem_limit_bytes=67_043_328
        ),
        name="afno",
    )(*ins)


def body(
    tokens, norm_gain, norm_shift, first_weight, first_bias, second_weight, second_bias, upstream
):
    wide = lambda v: jnp.broadcast_to(v[:, None], (CH, LON)).reshape(1, CH * LON)
    result, grad_tokens, params, ends = mega(
        tokens, upstream, wide(norm_gain), wide(norm_shift),
        big_matrix(first_weight), first_bias.reshape(2 * CH, 1),
        big_matrix(second_weight), second_bias.reshape(2 * CH, 1),
    )
    params = params.reshape(512, 128)[: 4 * CH].reshape(2, 2, 1, CH, 128)
    weights, biases = params[..., :CH], params[..., CH]
    return (
        result, grad_tokens, weights[0], biases[0], weights[1], biases[1],
        ends[:, 0, :GROUP].reshape(CH), ends[:, 1, :GROUP].reshape(CH),
    )


def solution(mesh):
    whole, weight, bias = P(None, "lat", "ch"), P(None, "ch", None, None), P(None, "ch", None)
    return jax.shard_map(
        body,
        mesh=mesh,
        in_specs=(whole, P("ch"), P("ch"), weight, bias, weight, bias, whole),
        out_specs=(whole, whole, weight, bias, weight, bias, P("ch"), P("ch")),
        check_vma=False,
    )
```

```python
import functools
import math

import jax
import jax.numpy as jnp
import numpy as np
from jax import lax
from jax.experimental import pallas as pl
from jax.experimental.pallas import tpu as pltpu
from jax.sharding import Mesh
from jax.sharding import PartitionSpec as P

LAT_ROWS = 64
LON = 180
MODES = 91
CH = 96
GROUP = 32
GROUPS = CH // GROUP
SPAN = GROUP * LON
PITCH = 40
EMBED = 768
layer_eps = 1e-05
shrink = 0.1
f32 = jnp.float32
bf16 = jnp.bfloat16


def split_table(table):
    high = table.astype(np.float32).astype(bf16)
    low = (table - high.astype(np.float64)).astype(np.float32).astype(bf16)
    return high, low


@functools.cache
def tables():
    m = np.arange(33)[:, None]
    h = np.arange(LAT_ROWS)[None, :]
    ang = 2.0 * np.pi * ((m * h) % LAT_ROWS) / LAT_ROWS
    lat = np.concatenate([np.cos(ang), np.sin(ang)[1:32]], axis=0) / math.sqrt(LAT_ROWS)
    w = np.arange(LON)[:, None]
    k = np.arange(MODES)[None, :]
    ang = 2.0 * np.pi * ((w * k) % LON) / LON
    lon = np.zeros((256, 256))
    lon[:LON, :MODES] = np.cos(ang) / math.sqrt(LON)
    lon[:LON, 128 : 128 + MODES] = np.sin(ang) / math.sqrt(LON)
    lon[:LON, 128 + MODES - 1] = 0.0
    lon[:LON, 128] = 0.0
    double = np.zeros((256,))
    double[:MODES] = 2.0
    double[128 : 128 + MODES] = 2.0
    double[[0, MODES - 1, 128, 128 + MODES - 1]] = 1.0
    return lat, lon, lon * double[None, :]


def split(x):
    high = x.astype(bf16)
    return high, (x - high.astype(f32)).astype(bf16)


def dot(a, b):
    return jnp.dot(a, b, preferred_element_type=f32)


def dot_nt(a, b):
    return lax.dot_general(a, b, (((1,), (1,)), ((), ())), preferred_element_type=f32)


STEP = 8


def gather_modes(re, im):
    return jnp.concatenate([jnp.concatenate([re[j], im[j]], axis=0) for j in range(STEP)], axis=1)


def lane_parts(ref_or_value):
    return [slice(c * LON, (c + 1) * LON) for c in range(GROUP)]


def widen(dst, values):
    for part in lane_parts(dst):
        dst[:, part] = values


def narrow(src):
    total = None
    for part in lane_parts(src):
        v = src[:, part]
        total = v if total is None else total + v
    return total


MESH = pl.DeviceIdType.MESH
UP, NORM, FILT, GRAD = range(4)


def mega_kernel(
    gain_s, shift_s, tokens, upstream, w1_ref, b1_ref, w2_ref, b2_ref,
    lat_ref, lonh, lonl, latih, latil, lonih, lonil,
    result, grad_tokens, params_out, ends_out,
    gain_x, shift_x, big, bias, bias_columns,
    tok, upr, cols, normed, filt, grad, spec, stash, zs, ya, yb, center, scale, first, second,
    sums_send, sums_recv, sums_all, wh, wl, wt, a1, a2, c1, c2, pack, packed_recv, piece, parts, ends_send, ends_recv,
    load_sem, store_sem, send_sem, recv_sem, ch_send, ch_recv, all_send, all_recv, small_send, small_recv,
):
    lat = lax.axis_index("lat")
    ch = lax.axis_index("ch")
    peers, chs = 32, 8

    def peer_at(s):
        return lax.rem(lat + 64 + ((s + 1) // 2) * (2 * lax.rem(s, 2) - 1), peers)

    def lanes(g):
        return pl.ds(pl.multiple_of(g * SPAN, SPAN), SPAN)

    def each_peer(fn):
        lax.fori_loop(1, peers, lambda s, z: (fn(peer_at(s)), z)[1], 0)

    def each_ch(fn):
        lax.fori_loop(1, chs, lambda s, z: (fn(lax.rem(ch + s, chs)), z)[1], 0)

    loads = [
        pltpu.make_async_copy(tokens, tok, load_sem.at[1]),
        pltpu.make_async_copy(upstream, upr, load_sem.at[0]),
    ]
    for c in loads:
        c.start()

    barrier = pltpu.get_barrier_semaphore()
    each_peer(lambda p: pl.semaphore_signal(barrier, inc=1, device_id={"lat": p}, device_id_type=MESH))
    each_ch(lambda p: pl.semaphore_signal(barrier, inc=1, device_id={"ch": p}, device_id_type=MESH))
    def rows_of(ref, g):
        return ref[:, :, lanes(g)].reshape(LAT_ROWS, SPAN).astype(f32)

    def put_rows(ref, g, value):
        ref[:, :, lanes(g)] = value.astype(bf16).reshape(32, 2, SPAN)

    first[...] = jnp.zeros_like(first)
    second[...] = jnp.zeros_like(second)
    loads[0].wait()

    @pl.loop(0, GROUPS)
    def _(g):
        x = rows_of(tok, g)
        first[...] += x
        second[...] += x * x

    pl.semaphore_wait(barrier, peers - 1 + chs - 1)

    def send_field(src, dst, kind, g):
        def go(p):
            pltpu.make_async_remote_copy(
                src_ref=src.at[p, :, lanes(g)],
                dst_ref=dst.at[lat, :, lanes(g)],
                send_sem=send_sem.at[kind, g],
                recv_sem=recv_sem.at[kind, g],
                device_id={"lat": p},
                device_id_type=MESH,
            ).start()

        each_peer(go)

    def wait_bytes(buf, sem):
        ref = buf.at[pl.ds(0, peers - 1)]
        pltpu.make_async_copy(ref, ref, sem).wait()

    def wait_field(buf, sem, kind, g):
        ref = buf.at[pl.ds(0, peers - 1), :, lanes(g)]
        pltpu.make_async_copy(ref, ref, sem.at[kind, g]).wait()

    def keep_own(src, dst, g):
        dst[lat, :, lanes(g)] = src[lat, :, lanes(g)]

    loads[1].wait()
    send_field(upr, cols.at[0], UP, 0)
    send_field(upr, cols.at[0], UP, 1)

    def rows8(p):
        return pl.ds(pl.multiple_of(p * 8, 8), 8)

    def over_channels(which):
        sums_send[which, :, 0:LON] = narrow(first)
        sums_send[which, :, LON : 2 * LON] = narrow(second)
        sums_send[which, :, 2 * LON :] = jnp.zeros((LAT_ROWS, 384 - 2 * LON), f32)
        sums_recv[which, ch] = sums_send[which, rows8(ch), :]

        def go(p):
            pltpu.make_async_remote_copy(
                src_ref=sums_send.at[which, rows8(p), :],
                dst_ref=sums_recv.at[which, ch],
                send_sem=ch_send.at[which],
                recv_sem=ch_recv.at[which],
                device_id={"ch": p},
                device_id_type=MESH,
            ).start()

        each_ch(go)

    def share_channels(which):
        ref = sums_recv.at[which, pl.ds(0, chs - 1)]
        pltpu.make_async_copy(ref, ref, ch_recv.at[which]).wait()
        total = sums_recv[which, 0]
        for p in range(1, chs):
            total = total + sums_recv[which, p]
        sums_all[which, ch] = total * (1.0 / EMBED)

        def go(p):
            pltpu.make_async_remote_copy(
                src_ref=sums_all.at[which, ch],
                dst_ref=sums_all.at[which, ch],
                send_sem=all_send.at[which],
                recv_sem=all_recv.at[which],
                device_id={"ch": p},
                device_id_type=MESH,
            ).start()

        each_ch(go)

    def wait_channels(which):
        ref = sums_all.at[which, pl.ds(0, chs - 1)]
        pltpu.make_async_copy(ref, ref, all_recv.at[which]).wait()
        return sums_all[which].reshape(LAT_ROWS, 384)

    over_channels(0)

    @pl.loop(0, GROUPS)
    def _(g):
        for source, wide in ((gain_s, gain_x), (shift_s, shift_x)):
            for c in range(GROUP):
                wide[g, :, c * LON : (c + 1) * LON] = jnp.full((1, LON), source[g * GROUP + c], f32)

    share_channels(0)
    ya[...] = jnp.zeros_like(ya)
    yb[...] = jnp.zeros_like(yb)
    bias[...] = jnp.zeros_like(bias)
    for n, (w_ref, b_ref) in enumerate(((w1_ref, b1_ref), (w2_ref, b2_ref))):
        real, imag = w_ref[0, 0], w_ref[1, 0]
        big[:CH, :CH] = real
        big[CH:, CH:] = real
        big[:CH, CH:] = imag
        big[CH:, :CH] = -imag
        matrix = big[...]
        wt[n] = matrix.astype(bf16)
        wh[n], wl[n] = split(matrix.T)
        bias[n : n + 1, 0:CH] = b_ref[0]
        bias[n : n + 1, CH : 2 * CH] = b_ref[1]
    for g in range(GROUPS):
        keep_own(upr, cols.at[0], g)
    for r in (a1, a2, c1, c2, pack, parts):
        r[...] = jnp.zeros_like(r)
    bias_columns[...] = bias[...].T
    sums = wait_channels(0)
    mean = sums[:, 0:LON]
    variance = sums[:, LON : 2 * LON] - mean * mean
    widen(center, mean)
    widen(scale, lax.rsqrt(variance + layer_eps))

    @pl.loop(0, GROUPS)
    def _(g):
        standard = (rows_of(tok, g) - center[...]) * scale[...]
        put_rows(normed, g, standard * gain_x[g] + shift_x[g])
        keep_own(normed, cols.at[1], g)
        send_field(normed, cols.at[1], NORM, g)

    send_field(upr, cols.at[0], UP, 2)

    def spectrum(field, g):
        x = cols[field, :, :, lanes(g)].reshape(LAT_ROWS, SPAN)
        both = dot(lat_ref[...], x)
        zs[...] = both[:LAT_ROWS] + both[LAT_ROWS:]
        for c in range(GROUP):
            v = zs[:, c * LON : (c + 1) * LON]
            ya[pl.ds(c, LAT_ROWS, stride=PITCH), :] = v[:, :128]
            yb[pl.ds(c, LAT_ROWS, stride=PITCH), 0 : LON - 128] = v[:, 128:]
        rows = jnp.concatenate([ya[...], yb[...]], axis=1)
        rows = rows.reshape(LAT_ROWS, PITCH, 256)[:, :GROUP].reshape(LAT_ROWS * GROUP, 256)
        high, low = split(rows)
        p = dot(high, lonh[field]) + dot(low, lonh[field]) + dot(high, lonl[field])
        p = p.reshape(LAT_ROWS, GROUP, 256)
        cc, cs = p[:, :, :128], p[:, :, 128:]
        here = pl.ds(pl.multiple_of(g * GROUP, GROUP), GROUP)
        re, im = spec.at[field, 0], spec.at[field, 1]
        re[0:1, here] = cc[0:1]
        im[0:1, here] = -cs[0:1]
        re[32:33, here] = cc[32:33]
        im[32:33, here] = -cs[32:33]
        re[1:32, here] = cc[1:32] - cs[33:64]
        re[33:64, here] = cc[1:32] + cs[33:64]
        im[1:32, here] = -cs[1:32] - cc[33:64]
        im[33:64, here] = cc[33:64] - cs[1:32]

    @pl.loop(0, 2)
    def _(g):
        wait_field(cols.at[0], recv_sem, UP, g)
        spectrum(0, g)

    @pl.loop(0, GROUPS)
    def _(g):
        wait_field(cols.at[1], recv_sem, NORM, g)
        spectrum(1, g)

    @pl.loop(0, LAT_ROWS // STEP)
    def _(i):
        at = pl.ds(i * STEP, STEP)
        re, im = spec.at[1, 0], spec.at[1, 1]
        xh, xl = split(gather_modes(re[at], im[at]))
        pre = dot(wh[0], xh) + dot(wh[0], xl) + dot(wl[0], xh) + bias_columns[: 2 * CH, 0:1]
        a = math.sqrt(2.0 / math.pi)
        sq = pre * pre
        th = jnp.tanh(a * pre * (1.0 + 0.044715 * sq))
        half = 0.5 * (1.0 + th)
        hid = pre * half
        slope = half + 0.5 * pre * (1.0 - th * th) * (a * (1.0 + 3.0 * 0.044715 * sq))
        hh, hl = split(hid)
        pre2 = dot(wh[1], hh) + dot(wh[1], hl) + dot(wl[1], hh) + bias_columns[: 2 * CH, 1:2]
        t = jnp.tanh(pre2 * (1.0 / shrink))
        mixed = pre2 - shrink * t
        for j in range(STEP):
            re[i * STEP + j] = mixed[:CH, 128 * j : 128 * (j + 1)]
            im[i * STEP + j] = mixed[CH:, 128 * j : 128 * (j + 1)]
        stash[0, i] = xh
        stash[1, i] = slope.astype(bf16)
        stash[2, i] = hh
        stash[3, i] = (t * t).astype(bf16)

    def field_of(field, g, dst):
        here = pl.ds(pl.multiple_of(g * GROUP, GROUP), GROUP)
        gr, gi = spec[field, 0, :, here], spec[field, 1, :, here]
        left = jnp.concatenate([gr[0:1], gr[1:32] + gr[33:64], gr[32:33], gi[33:64] - gi[1:32]], axis=0)
        right = -jnp.concatenate([gi[0:1], gi[1:32] + gi[33:64], gi[32:33], gr[1:32] - gr[33:64]], axis=0)
        rows = jnp.concatenate([left, right], axis=2).reshape(LAT_ROWS * GROUP, 256).astype(bf16)
        v = dot(rows, lonih[field]) + dot(rows, lonil[field])
        v = v.reshape(LAT_ROWS, GROUP, 256)
        va, vb = ya.reshape(LAT_ROWS, PITCH, 128), yb.reshape(LAT_ROWS, PITCH, 128)
        va[:, 0:GROUP, :] = v[:, :, :128]
        vb[:, 0:GROUP, :] = v[:, :, 128:]
        for c in range(GROUP):
            zs[:, c * LON : c * LON + 128] = ya[pl.ds(c, LAT_ROWS, stride=PITCH), :]
            zs[:, c * LON + 128 : (c + 1) * LON] = yb[pl.ds(c, LAT_ROWS, stride=PITCH), 0 : LON - 128]
        z = zs[...].astype(bf16)
        put_rows(dst, g, dot(latih[...], z) + dot(latil[...], z))

    @pl.loop(0, GROUPS)
    def _(g):
        field_of(1, g, cols.at[1])
        keep_own(cols.at[1], filt, g)
        send_field(cols.at[1], filt, FILT, g)

    wait_field(cols.at[0], recv_sem, UP, 2)
    yb[:, LON - 128 :] = jnp.zeros((LAT_ROWS * PITCH, 256 - LON), f32)
    spectrum(0, 2)

    @pl.loop(0, LAT_ROWS // STEP)
    def _(i):
        at = pl.ds(i * STEP, STEP)
        re, im = spec.at[0, 0], spec.at[0, 1]
        p2 = gather_modes(re[at], im[at]) * stash[3, i].astype(f32)
        p2h = p2.astype(bf16)
        p1 = dot(wt[1], p2h) * stash[1, i].astype(f32)
        p1h = p1.astype(bf16)
        out = dot(wt[0], p1h)
        for j in range(STEP):
            re[i * STEP + j] = out[:CH, 128 * j : 128 * (j + 1)]
            im[i * STEP + j] = out[CH:, 128 * j : 128 * (j + 1)]
        a2[...] += dot_nt(stash[2, i], p2h)
        a1[...] += dot_nt(stash[0, i], p1h)
        c2[...] += sum(p2[:, 128 * j : 128 * (j + 1)] for j in range(STEP))
        c1[...] += sum(p1[:, 128 * j : 128 * (j + 1)] for j in range(STEP))

    @pl.loop(0, GROUPS)
    def _(g):
        field_of(0, g, cols.at[0])
        keep_own(cols.at[0], grad, g)
        send_field(cols.at[0], grad, GRAD, g)

    for n, (acc, line) in enumerate(((a1, c1), (a2, c2))):
        v = acc[...]
        top = n * 2 * CH
        pack[top : top + CH, :CH] = v[:CH, :CH] + v[CH:, CH:]
        pack[top + CH : top + 2 * CH, :CH] = v[:CH, CH:] - v[CH:, :CH]
        row = jnp.sum(line[...].T, axis=0, keepdims=True)
        pack[4 * CH + 2 * n : 4 * CH + 2 * n + 1, :CH] = row[:, :CH]
        pack[4 * CH + 2 * n + 1 : 4 * CH + 2 * n + 2, :CH] = row[:, CH:]

    def rows16(p):
        return pl.ds(pl.multiple_of(p * 16, 16), 16)

    packed_recv[lat] = pack[rows16(lat), :]

    def send_piece(p):
        pltpu.make_async_remote_copy(
            src_ref=pack.at[rows16(p), :],
            dst_ref=packed_recv.at[lat],
            send_sem=small_send.at[0],
            recv_sem=small_recv.at[0],
            device_id={"lat": p},
            device_id_type=MESH,
        ).start()

    each_peer(send_piece)

    @pl.loop(0, GROUPS)
    def _(g):
        wait_field(filt, recv_sem, FILT, g)
        put_rows(filt, g, rows_of(tok, g) + rows_of(normed, g) + rows_of(filt, g))
        pltpu.make_async_copy(filt.at[:, :, lanes(g)], result.at[:, :, lanes(g)], store_sem.at[0, g]).start()

    first[...] = jnp.zeros_like(first)
    second[...] = jnp.zeros_like(second)

    def close_part(g):
        base = parts[:, lanes(g)]
        column = jnp.concatenate(
            [jnp.sum(base[:, c * LON : (c + 1) * LON], axis=1, keepdims=True) for c in range(GROUP)], axis=1
        )
        ends_send[g] = jnp.concatenate([column, jnp.zeros((8, 128 - GROUP), f32)], axis=1)

    @pl.loop(0, GROUPS)
    def _(g):
        @pl.when(g > 0)
        def _():
            close_part(g - 1)

        wait_field(grad, recv_sem, GRAD, g)
        standard = (rows_of(tok, g) - center[...]) * scale[...]
        total = rows_of(upr, g) + rows_of(grad, g)
        cross = total * standard
        gain = gain_x[g]
        first[...] += total * gain
        second[...] += cross * gain
        parts[0:1, lanes(g)] = jnp.sum(cross, axis=0, keepdims=True)
        parts[1:2, lanes(g)] = jnp.sum(total, axis=0, keepdims=True)

    over_channels(1)
    wait_bytes(packed_recv, small_recv.at[0])
    piece[...] = jnp.sum(packed_recv[...], axis=0)
    params_out[lat] = piece[...]

    def send_sum(p):
        pltpu.make_async_remote_copy(
            src_ref=piece,
            dst_ref=params_out.at[lat],
            send_sem=small_send.at[1],
            recv_sem=small_recv.at[1],
            device_id={"lat": p},
            device_id_type=MESH,
        ).start()

    each_peer(send_sum)
    share_channels(1)
    close_part(GROUPS - 1)
    ends_recv[lat] = ends_send[...]

    def send_ends(p):
        pltpu.make_async_remote_copy(
            src_ref=ends_send,
            dst_ref=ends_recv.at[lat],
            send_sem=small_send.at[2],
            recv_sem=small_recv.at[2],
            device_id={"lat": p},
            device_id_type=MESH,
        ).start()

    each_peer(send_ends)
    sums = wait_channels(1)
    widen(first, sums[:, 0:LON])
    widen(second, sums[:, LON : 2 * LON])

    @pl.loop(0, GROUPS)
    def _(g):
        inverse = scale[...]
        standard = (rows_of(tok, g) - center[...]) * inverse
        up = rows_of(upr, g)
        slope = (up + rows_of(grad, g)) * gain_x[g]
        put_rows(grad, g, up + inverse * (slope - first[...] - standard * second[...]))
        pltpu.make_async_copy(grad.at[:, :, lanes(g)], grad_tokens.at[:, :, lanes(g)], store_sem.at[1, g]).start()

    wait_bytes(ends_recv, small_recv.at[2])
    ends_out[...] = jnp.sum(ends_recv[...], axis=0)
    wait_bytes(params_out, small_recv.at[1])
    for which, buf, out in ((0, filt, result), (1, grad, grad_tokens)):
        for g in range(GROUPS):
            pltpu.make_async_copy(buf.at[:, :, lanes(g)], out.at[:, :, lanes(g)], store_sem.at[which, g]).wait()
    for kind, buf in ((UP, upr), (NORM, normed), (FILT, cols.at[1]), (GRAD, cols.at[0])):
        for g in range(GROUPS):
            wait_field(buf, send_sem, kind, g)
    for which in range(2):
        ref = sums_recv.at[which, pl.ds(0, chs - 1)]
        pltpu.make_async_copy(ref, ref, ch_send.at[which]).wait()
        ref = sums_all.at[which, pl.ds(0, chs - 1)]
        pltpu.make_async_copy(ref, ref, all_send.at[which]).wait()
    wait_bytes(packed_recv, small_send.at[0])
    wait_bytes(params_out, small_send.at[1])
    wait_bytes(ends_recv, small_send.at[2])


PIECES = 9


def finish_kernel(
    result, grad_tokens, params, ends, o_result, o_grad, fw, fb, sw, sb, og, os, hold, load_sem, store_sem
):
    width = CH * LON // PIECES
    pairs = ((result, o_result), (grad_tokens, o_grad))
    at = lambda ref, i: ref.at[:, :, i * width : (i + 1) * width]
    for i in range(PIECES):
        for n, (src, dst) in enumerate(pairs):
            pltpu.make_async_copy(at(src, i), at(hold.at[n], i), load_sem.at[n, i]).start()
    p = params[...].reshape(512, 128)
    for n, (weight, line) in enumerate(((fw, fb), (sw, sb))):
        for part in range(2):
            top = (2 * n + part) * CH
            weight[part, 0] = p[top : top + CH, :CH]
            line[part] = p[4 * CH + 2 * n + part : 4 * CH + 2 * n + part + 1, :CH]
    for g in range(GROUPS):
        og[:, g * GROUP : (g + 1) * GROUP] = ends[g, 0:1, :GROUP]
        os[:, g * GROUP : (g + 1) * GROUP] = ends[g, 1:2, :GROUP]
    for i in range(PIECES):
        for n, (src, dst) in enumerate(pairs):
            pltpu.make_async_copy(at(src, i), at(hold.at[n], i), load_sem.at[n, i]).wait()
            pltpu.make_async_copy(at(hold.at[n], i), at(dst, i), store_sem.at[n, i]).start()
    for i in range(PIECES):
        for n, (src, dst) in enumerate(pairs):
            pltpu.make_async_copy(at(hold.at[n], i), at(dst, i), store_sem.at[n, i]).wait()


def finish(result, grad_tokens, params, ends):
    hbm, vmem = pl.BlockSpec(memory_space=pl.ANY), pl.BlockSpec(memory_space=pltpu.VMEM)
    field = jax.ShapeDtypeStruct((32, 2, CH * LON), bf16)
    weight, line, vec = [jax.ShapeDtypeStruct(x, f32) for x in ((2, 1, CH, CH), (2, 1, CH), (1, CH))]
    return pl.pallas_call(
        finish_kernel,
        in_specs=[hbm, hbm, vmem, vmem],
        out_specs=[hbm, hbm] + [vmem] * 6,
        out_shape=[field, field, weight, line, weight, line, vec, vec],
        scratch_shapes=[
            pltpu.VMEM((2, 32, 2, CH * LON), bf16),
            pltpu.SemaphoreType.DMA((2, PIECES)), pltpu.SemaphoreType.DMA((2, PIECES)),
        ],
        compiler_params=pltpu.CompilerParams(vmem_limit_bytes=67_043_328),
        name="finish",
    )(result, grad_tokens, params, ends)


def mega(gain, shift, tokens, upstream, w1, b1, w2, b2):
    lat, lon, lon2 = tables()
    pair = lambda a, b: [jnp.asarray(np.stack(x)) for x in zip(split_table(a), split_table(b))]
    lat_h, lat_l = split_table(lat)
    lati_h, lati_l = split_table(lat.T)
    lonh, lonl = pair(lon2, lon)
    lonih, lonil = pair(lon.T, lon2.T)
    hbm, vmem = pl.BlockSpec(memory_space=pl.ANY), pl.BlockSpec(memory_space=pltpu.VMEM)
    smem = pl.BlockSpec(memory_space=pltpu.SMEM)
    field = jax.ShapeDtypeStruct((32, 2, CH * LON), bf16)
    V, D = pltpu.VMEM, pltpu.SemaphoreType.DMA
    fld = V((32, 2, CH * LON), bf16)
    wide = V((LAT_ROWS, SPAN), f32)
    ins = [
        gain, shift, tokens, upstream, w1, b1, w2, b2,
        jnp.asarray(np.concatenate([lat_h, lat_l], axis=0)), lonh, lonl,
        jnp.asarray(lati_h), jnp.asarray(lati_l), lonih, lonil,
    ]
    return pl.pallas_call(
        mega_kernel,
        in_specs=[smem, smem, hbm, hbm] + [vmem] * (len(ins) - 4),
        out_specs=[hbm, hbm, vmem, vmem],
        out_shape=[
            field, field,
            jax.ShapeDtypeStruct((32, 16, 128), f32),
            jax.ShapeDtypeStruct((GROUPS, 8, 128), f32),
        ],
        scratch_shapes=[
            V((GROUPS, 1, SPAN), f32), V((GROUPS, 1, SPAN), f32), V((192, 192), f32), V((8, 256), f32), V((256, 8), f32),
            fld, fld, V((2, 32, 2, CH * LON), bf16), fld, fld, fld,
            V((2, 2, LAT_ROWS, CH, 128), f32),
            V((4, LAT_ROWS // STEP, 2 * CH, 128 * STEP), bf16),
            wide, V((LAT_ROWS * PITCH, 128), f32), V((LAT_ROWS * PITCH, 128), f32),
            wide, wide, wide, wide,
            V((2, LAT_ROWS, 384), f32), V((2, 8, 8, 384), f32), V((2, 8, 8, 384), f32),
            V((2, 192, 192), bf16), V((2, 192, 192), bf16), V((2, 192, 192), bf16),
            V((192, 192), f32), V((192, 192), f32), V((192, 128), f32), V((192, 128), f32),
            V((512, 128), f32), V((32, 16, 128), f32), V((16, 128), f32),
            V((8, CH * LON), f32), V((GROUPS, 8, 128), f32), V((32, GROUPS, 8, 128), f32),
            D((2,)), D((2, GROUPS)), D((4, GROUPS)), D((4, GROUPS)), D((2,)), D((2,)), D((2,)), D((2,)), D((3,)), D((3,)),
        ],
        compiler_params=pltpu.CompilerParams(
            collective_id=0, has_side_effects=True, vmem_limit_bytes=67_043_328
        ),
        name="afno",
    )(*ins)


def body(
    tokens, norm_gain, norm_shift, first_weight, first_bias, second_weight, second_bias, upstream
):
    ends = mega(
        norm_gain, norm_shift, tokens, upstream, first_weight, first_bias, second_weight, second_bias
    )
    result, grad_tokens, fw, fb, sw, sb, gain, shift = finish(*ends)
    return result, grad_tokens, fw, fb, sw, sb, gain.reshape(CH), shift.reshape(CH)


def solution(mesh):
    whole, weight, bias = P(None, "lat", "ch"), P(None, "ch", None, None), P(None, "ch", None)
    return jax.shard_map(
        body,
        mesh=mesh,
        in_specs=(whole, P("ch"), P("ch"), weight, bias, weight, bias, whole),
        out_specs=(whole, whole, weight, bias, weight, bias, P("ch"), P("ch")),
        check_vma=False,
    )
```

```python
import functools
import math

import jax
import jax.numpy as jnp
import numpy as np
from jax import lax
from jax.experimental import pallas as pl
from jax.experimental.pallas import tpu as pltpu
from jax.sharding import Mesh
from jax.sharding import PartitionSpec as P

LAT_ROWS = 64
LON = 180
MODES = 91
CH = 96
GROUP = 32
GROUPS = CH // GROUP
SPAN = GROUP * LON
PITCH = 40
EMBED = 768
layer_eps = 1e-05
shrink = 0.1
f32 = jnp.float32
bf16 = jnp.bfloat16


def split_table(table):
    high = table.astype(np.float32).astype(bf16)
    low = (table - high.astype(np.float64)).astype(np.float32).astype(bf16)
    return high, low


@functools.cache
def tables():
    m = np.arange(33)[:, None]
    h = np.arange(LAT_ROWS)[None, :]
    ang = 2.0 * np.pi * ((m * h) % LAT_ROWS) / LAT_ROWS
    lat = np.concatenate([np.cos(ang), np.sin(ang)[1:32]], axis=0) / math.sqrt(LAT_ROWS)
    w = np.arange(LON)[:, None]
    k = np.arange(MODES)[None, :]
    ang = 2.0 * np.pi * ((w * k) % LON) / LON
    lon = np.zeros((256, 256))
    lon[:LON, :MODES] = np.cos(ang) / math.sqrt(LON)
    lon[:LON, 128 : 128 + MODES] = np.sin(ang) / math.sqrt(LON)
    lon[:LON, 128 + MODES - 1] = 0.0
    lon[:LON, 128] = 0.0
    double = np.zeros((256,))
    double[:MODES] = 2.0
    double[128 : 128 + MODES] = 2.0
    double[[0, MODES - 1, 128, 128 + MODES - 1]] = 1.0
    return lat, lon, lon * double[None, :]


def split(x):
    high = x.astype(bf16)
    return high, (x - high.astype(f32)).astype(bf16)


def dot(a, b):
    return jnp.dot(a, b, preferred_element_type=f32)


def dot_nt(a, b):
    return lax.dot_general(a, b, (((1,), (1,)), ((), ())), preferred_element_type=f32)


STEP = 8


def gather_modes(re, im):
    return jnp.concatenate([jnp.concatenate([re[j], im[j]], axis=0) for j in range(STEP)], axis=1)


def lane_parts(ref_or_value):
    return [slice(c * LON, (c + 1) * LON) for c in range(GROUP)]


def widen(dst, values):
    for part in lane_parts(dst):
        dst[:, part] = values


def narrow(src):
    total = None
    for part in lane_parts(src):
        v = src[:, part]
        total = v if total is None else total + v
    return total


MESH = pl.DeviceIdType.MESH
UP, NORM, FILT, GRAD = range(4)


def mega_kernel(
    gain_s, shift_s, tokens, upstream, w1_hbm, b1_hbm, w2_hbm, b2_hbm,
    lat_hbm, lonh_hbm, lonl_hbm, latih_hbm, latil_hbm, lonih_hbm, lonil_hbm,
    result, grad_tokens, params_out, ends_out,
    w1_ref, b1_ref, w2_ref, b2_ref, lat_ref, lonh, lonl, latih, latil, lonih, lonil, table_sem,
    gain_x, shift_x, big, bias, bias_columns,
    tok, upr, cols, away, normed, filt, grad, spec, stash, zs, ya, yb, center, scale, first, second,
    sums_send, sums_recv, sums_all, wh, wl, wt, a1, a2, c1, c2, pack, pack16, packed_recv, piece, parts, ends_send, ends_recv, mean_send, mean_recv,
    load_sem, store_sem, send_sem, recv_sem, ch_send, ch_recv, all_send, all_recv, small_send, small_recv,
):
    lat = lax.axis_index("lat")
    ch = lax.axis_index("ch")
    peers, chs = 32, 8

    def peer_at(s):
        return lax.rem(lat + 64 + ((s + 1) // 2) * (2 * lax.rem(s, 2) - 1), peers)

    def lanes(g):
        return pl.ds(pl.multiple_of(g * SPAN, SPAN), SPAN)

    def each_peer(fn):
        lax.fori_loop(1, peers, lambda s, z: (fn(peer_at(s)), z)[1], 0)

    def each_ch(fn):
        lax.fori_loop(1, chs, lambda s, z: (fn(lax.rem(ch + s, chs)), z)[1], 0)

    barrier = pltpu.get_barrier_semaphore()
    each_peer(lambda p: pl.semaphore_signal(barrier, inc=1, device_id={"lat": p}, device_id_type=MESH))
    each_ch(lambda p: pl.semaphore_signal(barrier, inc=1, device_id={"ch": p}, device_id_type=MESH))
    loads = [
        pltpu.make_async_copy(upstream, upr, load_sem.at[0]),
        pltpu.make_async_copy(tokens, tok, load_sem.at[1]),
    ]
    for c in loads:
        c.start()

    sources = (
        (w1_hbm, w1_ref), (b1_hbm, b1_ref), (w2_hbm, w2_ref), (b2_hbm, b2_ref), (lat_hbm, lat_ref),
        (lonh_hbm, lonh), (lonl_hbm, lonl), (latih_hbm, latih), (latil_hbm, latil),
        (lonih_hbm, lonih), (lonil_hbm, lonil),
    )
    table_loads = [pltpu.make_async_copy(src, dst, table_sem.at[n]) for n, (src, dst) in enumerate(sources)]
    for c in table_loads:
        c.start()

    pl.semaphore_wait(barrier, peers - 1 + chs - 1)

    def rows_of(ref, g):
        return ref[:, :, lanes(g)].reshape(LAT_ROWS, SPAN).astype(f32)

    def put_rows(ref, g, value):
        ref[:, :, lanes(g)] = value.astype(bf16).reshape(32, 2, SPAN)

    def send_field(src, dst, kind, g):
        def go(p):
            pltpu.make_async_remote_copy(
                src_ref=src.at[p, :, lanes(g)],
                dst_ref=dst.at[lat, :, lanes(g)],
                send_sem=send_sem.at[kind, g],
                recv_sem=recv_sem.at[kind, g],
                device_id={"lat": p},
                device_id_type=MESH,
            ).start()

        each_peer(go)

    def wait_bytes(buf, sem):
        ref = buf.at[pl.ds(0, peers - 1)]
        pltpu.make_async_copy(ref, ref, sem).wait()

    def wait_field(buf, sem, kind, g):
        ref = buf.at[pl.ds(0, peers - 1), :, lanes(g)]
        pltpu.make_async_copy(ref, ref, sem.at[kind, g]).wait()

    def keep_own(src, dst, g):
        dst[lat, :, lanes(g)] = src[lat, :, lanes(g)]

    loads[0].wait()
    send_field(upr, cols.at[0], UP, 0)
    send_field(upr, cols.at[0], UP, 1)
    first[...] = jnp.zeros_like(first)
    second[...] = jnp.zeros_like(second)
    loads[1].wait()

    @pl.loop(0, GROUPS)
    def _(g):
        x = rows_of(tok, g)
        first[...] += x
        second[...] += x * x

    def rows8(p):
        return pl.ds(pl.multiple_of(p * 8, 8), 8)

    def over_channels(which):
        sums_send[which, :, 0:LON] = narrow(first)
        sums_send[which, :, LON : 2 * LON] = narrow(second)
        sums_send[which, :, 2 * LON :] = jnp.zeros((LAT_ROWS, 384 - 2 * LON), f32)
        sums_recv[which, ch] = sums_send[which, rows8(ch), :]

        def go(p):
            pltpu.make_async_remote_copy(
                src_ref=sums_send.at[which, rows8(p), :],
                dst_ref=sums_recv.at[which, ch],
                send_sem=ch_send.at[which],
                recv_sem=ch_recv.at[which],
                device_id={"ch": p},
                device_id_type=MESH,
            ).start()

        each_ch(go)

    def share_channels(which):
        ref = sums_recv.at[which, pl.ds(0, chs - 1)]
        pltpu.make_async_copy(ref, ref, ch_recv.at[which]).wait()
        total = sums_recv[which, 0]
        for p in range(1, chs):
            total = total + sums_recv[which, p]
        sums_all[which, ch] = total * (1.0 / EMBED)

        def go(p):
            pltpu.make_async_remote_copy(
                src_ref=sums_all.at[which, ch],
                dst_ref=sums_all.at[which, ch],
                send_sem=all_send.at[which],
                recv_sem=all_recv.at[which],
                device_id={"ch": p},
                device_id_type=MESH,
            ).start()

        each_ch(go)

    def wait_channels(which):
        ref = sums_all.at[which, pl.ds(0, chs - 1)]
        pltpu.make_async_copy(ref, ref, all_recv.at[which]).wait()
        return sums_all[which].reshape(LAT_ROWS, 384)

    over_channels(0)

    @pl.loop(0, GROUPS)
    def _(g):
        for source, wide in ((gain_s, gain_x), (shift_s, shift_x)):
            for c in range(GROUP):
                wide[g, :, c * LON : (c + 1) * LON] = jnp.full((1, LON), source[g * GROUP + c], f32)

    share_channels(0)
    for c in table_loads:
        c.wait()
    ya[...] = jnp.zeros_like(ya)
    yb[...] = jnp.zeros_like(yb)
    bias[...] = jnp.zeros_like(bias)
    for n, (w_ref, b_ref) in enumerate(((w1_ref, b1_ref), (w2_ref, b2_ref))):
        real, imag = w_ref[0, 0], w_ref[1, 0]
        big[:CH, :CH] = real
        big[CH:, CH:] = real
        big[:CH, CH:] = imag
        big[CH:, :CH] = -imag
        matrix = big[...]
        wt[n] = matrix.astype(bf16)
        wh[n], wl[n] = split(matrix.T)
        bias[n : n + 1, 0:CH] = b_ref[0]
        bias[n : n + 1, CH : 2 * CH] = b_ref[1]
    for g in range(GROUPS):
        keep_own(upr, cols.at[0], g)
    for r in (a1, a2, c1, c2, pack, parts):
        r[...] = jnp.zeros_like(r)
    bias_columns[...] = bias[...].T
    sums = wait_channels(0)
    mean = sums[:, 0:LON]
    variance = sums[:, LON : 2 * LON] - mean * mean
    widen(center, mean)
    widen(scale, lax.rsqrt(variance + layer_eps))

    @pl.loop(0, GROUPS)
    def _(g):
        standard = (rows_of(tok, g) - center[...]) * scale[...]
        put_rows(normed, g, standard * gain_x[g] + shift_x[g])
        keep_own(normed, cols.at[1], g)
        send_field(normed, cols.at[1], NORM, g)

    send_field(upr, cols.at[0], UP, 2)

    def spectrum(field, g):
        x = cols[field, :, :, lanes(g)].reshape(LAT_ROWS, SPAN)
        both = dot(lat_ref[...], x)
        zs[...] = both[:LAT_ROWS] + both[LAT_ROWS:]
        for c in range(GROUP):
            v = zs[:, c * LON : (c + 1) * LON]
            ya[pl.ds(c, LAT_ROWS, stride=PITCH), :] = v[:, :128]
            yb[pl.ds(c, LAT_ROWS, stride=PITCH), 0 : LON - 128] = v[:, 128:]
        rows = jnp.concatenate([ya[...], yb[...]], axis=1)
        rows = rows.reshape(LAT_ROWS, PITCH, 256)[:, :GROUP].reshape(LAT_ROWS * GROUP, 256)
        high, low = split(rows)
        p = dot(high, lonh[field]) + dot(low, lonh[field]) + dot(high, lonl[field])
        p = p.reshape(LAT_ROWS, GROUP, 256)
        cc, cs = p[:, :, :128], p[:, :, 128:]
        here = pl.ds(pl.multiple_of(g * GROUP, GROUP), GROUP)
        re, im = spec.at[field, 0], spec.at[field, 1]
        re[0:1, here] = cc[0:1]
        im[0:1, here] = -cs[0:1]
        re[32:33, here] = cc[32:33]
        im[32:33, here] = -cs[32:33]
        re[1:32, here] = cc[1:32] - cs[33:64]
        re[33:64, here] = cc[1:32] + cs[33:64]
        im[1:32, here] = -cs[1:32] - cc[33:64]
        im[33:64, here] = cc[33:64] - cs[1:32]

    @pl.loop(0, 2)
    def _(g):
        wait_field(cols.at[0], recv_sem, UP, g)
        spectrum(0, g)

    @pl.loop(0, GROUPS)
    def _(g):
        wait_field(cols.at[1], recv_sem, NORM, g)
        spectrum(1, g)

    @pl.loop(0, LAT_ROWS // STEP)
    def _(i):
        at = pl.ds(i * STEP, STEP)
        re, im = spec.at[1, 0], spec.at[1, 1]
        xh, xl = split(gather_modes(re[at], im[at]))
        pre = dot(wh[0], xh) + dot(wh[0], xl) + dot(wl[0], xh) + bias_columns[: 2 * CH, 0:1]
        a = math.sqrt(2.0 / math.pi)
        sq = pre * pre
        th = jnp.tanh(a * pre * (1.0 + 0.044715 * sq))
        half = 0.5 * (1.0 + th)
        hid = pre * half
        slope = half + 0.5 * pre * (1.0 - th * th) * (a * (1.0 + 3.0 * 0.044715 * sq))
        hh, hl = split(hid)
        pre2 = dot(wh[1], hh) + dot(wh[1], hl) + dot(wl[1], hh) + bias_columns[: 2 * CH, 1:2]
        t = jnp.tanh(pre2 * (1.0 / shrink))
        mixed = pre2 - shrink * t
        for j in range(STEP):
            re[i * STEP + j] = mixed[:CH, 128 * j : 128 * (j + 1)]
            im[i * STEP + j] = mixed[CH:, 128 * j : 128 * (j + 1)]
        stash[0, i] = xh
        stash[1, i] = slope.astype(bf16)
        stash[2, i] = hh
        stash[3, i] = (t * t).astype(bf16)

    def field_of(field, g):
        here = pl.ds(pl.multiple_of(g * GROUP, GROUP), GROUP)
        gr, gi = spec[field, 0, :, here], spec[field, 1, :, here]
        left = jnp.concatenate([gr[0:1], gr[1:32] + gr[33:64], gr[32:33], gi[33:64] - gi[1:32]], axis=0)
        right = -jnp.concatenate([gi[0:1], gi[1:32] + gi[33:64], gi[32:33], gr[1:32] - gr[33:64]], axis=0)
        rows = jnp.concatenate([left, right], axis=2).reshape(LAT_ROWS * GROUP, 256).astype(bf16)
        v = dot(rows, lonih[field]) + dot(rows, lonil[field])
        v = v.reshape(LAT_ROWS, GROUP, 256)
        va, vb = ya.reshape(LAT_ROWS, PITCH, 128), yb.reshape(LAT_ROWS, PITCH, 128)
        va[:, 0:GROUP, :] = v[:, :, :128]
        vb[:, 0:GROUP, :] = v[:, :, 128:]
        for c in range(GROUP):
            zs[:, c * LON : c * LON + 128] = ya[pl.ds(c, LAT_ROWS, stride=PITCH), :]
            zs[:, c * LON + 128 : (c + 1) * LON] = yb[pl.ds(c, LAT_ROWS, stride=PITCH), 0 : LON - 128]
        z = zs[...].astype(bf16)
        return dot(latih[...], z) + dot(latil[...], z)

    @pl.loop(0, GROUPS)
    def _(g):
        put_rows(away, g, field_of(1, g))
        keep_own(away, filt, g)
        send_field(away, filt, FILT, g)

    wait_field(cols.at[0], recv_sem, UP, 2)
    yb[:, LON - 128 :] = jnp.zeros((LAT_ROWS * PITCH, 256 - LON), f32)
    spectrum(0, 2)

    @pl.loop(0, LAT_ROWS // STEP)
    def _(i):
        at = pl.ds(i * STEP, STEP)
        re, im = spec.at[0, 0], spec.at[0, 1]
        p2 = gather_modes(re[at], im[at]) * stash[3, i].astype(f32)
        p2h = p2.astype(bf16)
        p1 = dot(wt[1], p2h) * stash[1, i].astype(f32)
        p1h = p1.astype(bf16)
        out = dot(wt[0], p1h)
        for j in range(STEP):
            re[i * STEP + j] = out[:CH, 128 * j : 128 * (j + 1)]
            im[i * STEP + j] = out[CH:, 128 * j : 128 * (j + 1)]
        a2[...] += dot_nt(stash[2, i], p2h)
        a1[...] += dot_nt(stash[0, i], p1h)
        c2[...] += sum(p2[:, 128 * j : 128 * (j + 1)] for j in range(STEP))
        c1[...] += sum(p1[:, 128 * j : 128 * (j + 1)] for j in range(STEP))

    for n, (acc, line) in enumerate(((a1, c1), (a2, c2))):
        v = acc[...]
        top = n * 2 * CH
        pack[top : top + CH, :CH] = v[:CH, :CH] + v[CH:, CH:]
        pack[top + CH : top + 2 * CH, :CH] = v[:CH, CH:] - v[CH:, :CH]
        row = jnp.sum(line[...].T, axis=0, keepdims=True)
        pack[4 * CH + 2 * n : 4 * CH + 2 * n + 1, :CH] = row[:, :CH]
        pack[4 * CH + 2 * n + 1 : 4 * CH + 2 * n + 2, :CH] = row[:, CH:]

    pack16[...] = pack[...].astype(bf16)

    def rows16(p):
        return pl.ds(pl.multiple_of(p * 16, 16), 16)

    packed_recv[lat] = pack16[rows16(lat), :]

    def send_piece(p):
        pltpu.make_async_remote_copy(
            src_ref=pack16.at[rows16(p), :],
            dst_ref=packed_recv.at[lat],
            send_sem=small_send.at[0],
            recv_sem=small_recv.at[0],
            device_id={"lat": p},
            device_id_type=MESH,
        ).start()

    each_peer(send_piece)

    first[...] = jnp.zeros_like(first)
    second[...] = jnp.zeros_like(second)

    @pl.loop(0, GROUPS)
    def _(g):
        out = field_of(0, g).astype(bf16)
        total = rows_of(cols.at[0], g) + out.astype(f32)
        first[...] += total * gain_x[g]
        second[...] += total * (rows_of(cols.at[1], g) - shift_x[g])
        put_rows(cols.at[0], g, out)
        keep_own(cols.at[0], grad, g)

        @pl.when(g < GROUPS - 1)
        def _():
            send_field(cols.at[0], grad, GRAD, g)

    over_channels(1)
    share_channels(1)
    mean_send[...] = wait_channels(1).reshape(32, 2, 384)
    mean_recv[lat] = mean_send[lat]

    def send_mean(p):
        pltpu.make_async_remote_copy(
            src_ref=mean_send.at[p],
            dst_ref=mean_recv.at[lat],
            send_sem=small_send.at[3],
            recv_sem=small_recv.at[3],
            device_id={"lat": p},
            device_id_type=MESH,
        ).start()

    each_peer(send_mean)
    send_field(cols.at[0], grad, GRAD, GROUPS - 1)

    @pl.loop(0, GROUPS)
    def _(g):
        wait_field(filt, recv_sem, FILT, g)
        put_rows(filt, g, rows_of(tok, g) + rows_of(normed, g) + rows_of(filt, g))
        pltpu.make_async_copy(filt.at[:, :, lanes(g)], result.at[:, :, lanes(g)], store_sem.at[0, g]).start()

    wait_bytes(packed_recv, small_recv.at[0])
    piece[...] = jnp.sum(packed_recv[...].astype(f32), axis=0).astype(bf16)
    params_out[lat] = piece[...]

    def send_sum(p):
        pltpu.make_async_remote_copy(
            src_ref=piece,
            dst_ref=params_out.at[lat],
            send_sem=small_send.at[1],
            recv_sem=small_recv.at[1],
            device_id={"lat": p},
            device_id_type=MESH,
        ).start()

    each_peer(send_sum)

    wait_bytes(mean_recv, small_recv.at[3])
    means = mean_recv[...].reshape(LAT_ROWS, 384)
    widen(first, means[:, 0:LON])
    widen(second, means[:, LON : 2 * LON])

    def close_part(g):
        base = parts[:, g * SPAN : (g + 1) * SPAN]
        column = jnp.concatenate(
            [jnp.sum(base[:, c * LON : (c + 1) * LON], axis=1, keepdims=True) for c in range(GROUP)], axis=1
        )
        ends_send[:, g * GROUP : (g + 1) * GROUP] = column[0:2]

    ends_send[...] = jnp.zeros_like(ends_send)

    @pl.loop(0, GROUPS)
    def _(g):
        for k in range(GROUPS - 1):
            pl.when(g == k + 1)(functools.partial(close_part, k))
        wait_field(grad, recv_sem, GRAD, g)
        inverse = scale[...]
        standard = (rows_of(tok, g) - center[...]) * inverse
        up = rows_of(upr, g)
        total = up + rows_of(grad, g)
        parts[0:1, lanes(g)] = jnp.sum(total * standard, axis=0, keepdims=True)
        parts[1:2, lanes(g)] = jnp.sum(total, axis=0, keepdims=True)
        slope = total * gain_x[g]
        put_rows(grad, g, up + inverse * (slope - first[...] - standard * second[...]))
        pltpu.make_async_copy(grad.at[:, :, lanes(g)], grad_tokens.at[:, :, lanes(g)], store_sem.at[1, g]).start()

    close_part(GROUPS - 1)
    ends_recv[lat] = ends_send[...]

    def send_ends(p):
        pltpu.make_async_remote_copy(
            src_ref=ends_send,
            dst_ref=ends_recv.at[lat],
            send_sem=small_send.at[2],
            recv_sem=small_recv.at[2],
            device_id={"lat": p},
            device_id_type=MESH,
        ).start()

    each_peer(send_ends)
    wait_bytes(ends_recv, small_recv.at[2])
    ends_out[...] = jnp.sum(ends_recv[...], axis=0)
    wait_bytes(params_out, small_recv.at[1])
    for which, buf, out in ((0, filt, result), (1, grad, grad_tokens)):
        for g in range(GROUPS):
            pltpu.make_async_copy(buf.at[:, :, lanes(g)], out.at[:, :, lanes(g)], store_sem.at[which, g]).wait()
    for kind, buf in ((UP, upr), (NORM, normed), (FILT, away), (GRAD, cols.at[0])):
        for g in range(GROUPS):
            wait_field(buf, send_sem, kind, g)
    for which in range(2):
        ref = sums_recv.at[which, pl.ds(0, chs - 1)]
        pltpu.make_async_copy(ref, ref, ch_send.at[which]).wait()
        ref = sums_all.at[which, pl.ds(0, chs - 1)]
        pltpu.make_async_copy(ref, ref, all_send.at[which]).wait()
    wait_bytes(packed_recv, small_send.at[0])
    wait_bytes(params_out, small_send.at[1])
    wait_bytes(ends_recv, small_send.at[2])
    wait_bytes(mean_recv, small_send.at[3])


PIECES = 9


def finish_kernel(
    result, grad_tokens, params, ends, o_result, o_grad, o_fw, o_fb, o_sw, o_sb, o_og, o_os,
    hold, params_v, ends_v, fw, fb, sw, sb, og, os, load_sem, store_sem, small_load, small_store,
):
    width = CH * LON // PIECES
    pairs = ((result, o_result), (grad_tokens, o_grad))
    at = lambda ref, i: ref.at[:, :, i * width : (i + 1) * width]
    small = [
        pltpu.make_async_copy(params, params_v, small_load.at[0]),
        pltpu.make_async_copy(ends, ends_v, small_load.at[1]),
    ]
    loads = [
        [pltpu.make_async_copy(at(src, i), at(hold.at[n], i), load_sem.at[n, i]) for n, (src, _) in enumerate(pairs)]
        for i in range(PIECES)
    ]
    stores = [
        [pltpu.make_async_copy(at(hold.at[n], i), at(dst, i), store_sem.at[n, i]) for n, (_, dst) in enumerate(pairs)]
        for i in range(PIECES)
    ]
    for c in small + sum(loads, []):
        c.start()
    for c in small:
        c.wait()
    p = params_v[...].astype(f32).reshape(512, 128)
    for n, (weight, line) in enumerate(((fw, fb), (sw, sb))):
        for part in range(2):
            top = (2 * n + part) * CH
            weight[part, 0] = p[top : top + CH, :CH]
            line[part] = p[4 * CH + 2 * n + part : 4 * CH + 2 * n + part + 1, :CH]
    og[...] = ends_v[0:1, :CH]
    os[...] = ends_v[1:2, :CH]
    outs = ((fw, o_fw), (fb, o_fb), (sw, o_sw), (sb, o_sb), (og, o_og), (os, o_os))
    small = [pltpu.make_async_copy(src, dst, small_store.at[n]) for n, (src, dst) in enumerate(outs)]
    for c in small:
        c.start()
    for i in range(PIECES):
        for n in range(2):
            loads[i][n].wait()
            stores[i][n].start()
    for c in small + sum(stores, []):
        c.wait()


def finish(result, grad_tokens, params, ends):
    hbm = pl.BlockSpec(memory_space=pl.ANY)
    field = jax.ShapeDtypeStruct((32, 2, CH * LON), bf16)
    weight, line, vec = [jax.ShapeDtypeStruct(x, f32) for x in ((2, 1, CH, CH), (2, 1, CH), (1, CH))]
    small = [weight, line, weight, line, vec, vec]
    return pl.pallas_call(
        finish_kernel,
        in_specs=[hbm] * 4,
        out_specs=[hbm] * 8,
        out_shape=[field, field] + small,
        scratch_shapes=[
            pltpu.VMEM((2, 32, 2, CH * LON), bf16),
            *[pltpu.VMEM(x.shape, x.dtype) for x in (params, ends, *small)],
            pltpu.SemaphoreType.DMA((2, PIECES)), pltpu.SemaphoreType.DMA((2, PIECES)),
            pltpu.SemaphoreType.DMA((2,)), pltpu.SemaphoreType.DMA((6,)),
        ],
        compiler_params=pltpu.CompilerParams(vmem_limit_bytes=67_043_328),
        name="finish",
    )(result, grad_tokens, params, ends)


def mega(gain, shift, tokens, upstream, w1, b1, w2, b2):
    lat, lon, lon2 = tables()
    pair = lambda a, b: [jnp.asarray(np.stack(x)) for x in zip(split_table(a), split_table(b))]
    lat_h, lat_l = split_table(lat)
    lati_h, lati_l = split_table(lat.T)
    lonh, lonl = pair(lon2, lon)
    lonih, lonil = pair(lon.T, lon2.T)
    hbm, vmem = pl.BlockSpec(memory_space=pl.ANY), pl.BlockSpec(memory_space=pltpu.VMEM)
    smem = pl.BlockSpec(memory_space=pltpu.SMEM)
    field = jax.ShapeDtypeStruct((32, 2, CH * LON), bf16)
    V, D = pltpu.VMEM, pltpu.SemaphoreType.DMA
    fld = V((32, 2, CH * LON), bf16)
    wide = V((LAT_ROWS, SPAN), f32)
    ins = [
        gain, shift, tokens, upstream, w1, b1, w2, b2,
        jnp.asarray(np.concatenate([lat_h, lat_l], axis=0)), lonh, lonl,
        jnp.asarray(lati_h), jnp.asarray(lati_l), lonih, lonil,
    ]
    return pl.pallas_call(
        mega_kernel,
        in_specs=[smem, smem] + [hbm] * (len(ins) - 2),
        out_specs=[hbm, hbm, vmem, vmem],
        out_shape=[
            field, field,
            jax.ShapeDtypeStruct((32, 16, 128), bf16),
            jax.ShapeDtypeStruct((2, 128), f32),
        ],
        scratch_shapes=[
            *[V(x.shape, x.dtype) for x in ins[4:]], D((len(ins) - 4,)),
            V((GROUPS, 1, SPAN), f32), V((GROUPS, 1, SPAN), f32), V((192, 192), f32), V((8, 256), f32), V((256, 8), f32),
            fld, fld, V((2, 32, 2, CH * LON), bf16), fld, fld, fld, fld,
            V((2, 2, LAT_ROWS, CH, 128), f32),
            V((4, LAT_ROWS // STEP, 2 * CH, 128 * STEP), bf16),
            wide, V((LAT_ROWS * PITCH, 128), f32), V((LAT_ROWS * PITCH, 128), f32),
            wide, wide, wide, wide,
            V((2, LAT_ROWS, 384), f32), V((2, 8, 8, 384), f32), V((2, 8, 8, 384), f32),
            V((2, 192, 192), bf16), V((2, 192, 192), bf16), V((2, 192, 192), bf16),
            V((192, 192), f32), V((192, 192), f32), V((192, 128), f32), V((192, 128), f32),
            V((512, 128), f32), V((512, 128), bf16), V((32, 16, 128), bf16), V((16, 128), bf16),
            V((8, CH * LON), f32), V((2, 128), f32), V((32, 2, 128), f32), V((32, 2, 384), f32), V((32, 2, 384), f32),
            D((2,)), D((2, GROUPS)), D((4, GROUPS)), D((4, GROUPS)), D((2,)), D((2,)), D((2,)), D((2,)), D((4,)), D((4,)),
        ],
        compiler_params=pltpu.CompilerParams(
            collective_id=0, has_side_effects=True, vmem_limit_bytes=67_043_328
        ),
        name="afno",
    )(*ins)


def body(
    tokens, norm_gain, norm_shift, first_weight, first_bias, second_weight, second_bias, upstream
):
    ends = mega(
        norm_gain, norm_shift, tokens, upstream, first_weight, first_bias, second_weight, second_bias
    )
    result, grad_tokens, fw, fb, sw, sb, gain, shift = finish(*ends)
    return result, grad_tokens, fw, fb, sw, sb, gain.reshape(CH), shift.reshape(CH)


def solution(mesh):
    whole, weight, bias = P(None, "lat", "ch"), P(None, "ch", None, None), P(None, "ch", None)
    return jax.shard_map(
        body,
        mesh=mesh,
        in_specs=(whole, P("ch"), P("ch"), weight, bias, weight, bias, whole),
        out_specs=(whole, whole, weight, bias, weight, bias, P("ch"), P("ch")),
        check_vma=False,
    )
```

```python
import functools
import math

import jax
import jax.numpy as jnp
import numpy as np
from jax import lax
from jax.experimental import pallas as pl
from jax.experimental.pallas import tpu as pltpu
from jax.sharding import Mesh
from jax.sharding import PartitionSpec as P

LAT_ROWS = 64
LON = 180
MODES = 91
CH = 96
GROUP = 32
GROUPS = CH // GROUP
SPAN = GROUP * LON
PITCH = 40
EMBED = 768
layer_eps = 1e-05
shrink = 0.1
f32 = jnp.float32
bf16 = jnp.bfloat16


def split_table(table):
    high = table.astype(np.float32).astype(bf16)
    low = (table - high.astype(np.float64)).astype(np.float32).astype(bf16)
    return high, low


@functools.cache
def tables():
    m = np.arange(33)[:, None]
    h = np.arange(LAT_ROWS)[None, :]
    ang = 2.0 * np.pi * ((m * h) % LAT_ROWS) / LAT_ROWS
    lat = np.concatenate([np.cos(ang), np.sin(ang)[1:32]], axis=0) / math.sqrt(LAT_ROWS)
    w = np.arange(LON)[:, None]
    k = np.arange(MODES)[None, :]
    ang = 2.0 * np.pi * ((w * k) % LON) / LON
    lon = np.zeros((256, 256))
    lon[:LON, :MODES] = np.cos(ang) / math.sqrt(LON)
    lon[:LON, 128 : 128 + MODES] = np.sin(ang) / math.sqrt(LON)
    lon[:LON, 128 + MODES - 1] = 0.0
    lon[:LON, 128] = 0.0
    double = np.zeros((256,))
    double[:MODES] = 2.0
    double[128 : 128 + MODES] = 2.0
    double[[0, MODES - 1, 128, 128 + MODES - 1]] = 1.0
    return lat, lon, lon * double[None, :]


def split(x):
    high = x.astype(bf16)
    return high, (x - high.astype(f32)).astype(bf16)


def dot(a, b):
    return jnp.dot(a, b, preferred_element_type=f32)


def dot_nt(a, b):
    return lax.dot_general(a, b, (((1,), (1,)), ((), ())), preferred_element_type=f32)


STEP = 8


def gather_modes(re, im):
    return jnp.concatenate([jnp.concatenate([re[j], im[j]], axis=0) for j in range(STEP)], axis=1)


def lane_parts(ref_or_value):
    return [slice(c * LON, (c + 1) * LON) for c in range(GROUP)]


def widen(dst, values):
    for part in lane_parts(dst):
        dst[:, part] = values


def narrow(src):
    total = None
    for part in lane_parts(src):
        v = src[:, part]
        total = v if total is None else total + v
    return total


MESH = pl.DeviceIdType.MESH
UP, NORM, FILT, GRAD = range(4)


def mega_kernel(
    gain_hbm, shift_hbm, tokens, upstream, w1_hbm, b1_hbm, w2_hbm, b2_hbm,
    lat_hbm, lonh_hbm, lonl_hbm, latih_hbm, latil_hbm, lonih_hbm, lonil_hbm,
    result, grad_tokens, params_out, ends_out,
    w1_ref, b1_ref, w2_ref, b2_ref, lat_ref, lonh, lonl, latih, latil, lonih, lonil, gain_s, shift_s, table_sem,
    gain_x, shift_x, big, bias, bias_columns,
    tok, upr, cols, away, normed, filt, grad, spec, stash, zs, ya, yb, center, scale, first, second,
    sums_send, sums_recv, sums_all, wh, wl, wt, a1, a2, c1, c2, pack, pack16, packed_recv, piece, parts, ends_send, ends_recv, mean_send, mean_recv,
    load_sem, store_sem, send_sem, recv_sem, ch_send, ch_recv, all_send, all_recv, small_send, small_recv,
):
    lat = lax.axis_index("lat")
    ch = lax.axis_index("ch")
    peers, chs = 32, 8

    def peer_at(s):
        return lax.rem(lat + 64 + ((s + 1) // 2) * (2 * lax.rem(s, 2) - 1), peers)

    def lanes(g):
        return pl.ds(pl.multiple_of(g * SPAN, SPAN), SPAN)

    def each_peer(fn):
        lax.fori_loop(1, peers, lambda s, z: (fn(peer_at(s)), z)[1], 0)

    def each_ch(fn):
        lax.fori_loop(1, chs, lambda s, z: (fn(lax.rem(ch + s, chs)), z)[1], 0)

    barrier = pltpu.get_barrier_semaphore()
    each_peer(lambda p: pl.semaphore_signal(barrier, inc=1, device_id={"lat": p}, device_id_type=MESH))
    each_ch(lambda p: pl.semaphore_signal(barrier, inc=1, device_id={"ch": p}, device_id_type=MESH))
    loads = [
        pltpu.make_async_copy(upstream, upr, load_sem.at[0]),
        pltpu.make_async_copy(tokens, tok, load_sem.at[1]),
    ]
    for c in loads:
        c.start()

    sources = (
        (w1_hbm, w1_ref), (b1_hbm, b1_ref), (w2_hbm, w2_ref), (b2_hbm, b2_ref), (lat_hbm, lat_ref),
        (lonh_hbm, lonh), (lonl_hbm, lonl), (latih_hbm, latih), (latil_hbm, latil),
        (lonih_hbm, lonih), (lonil_hbm, lonil), (gain_hbm, gain_s), (shift_hbm, shift_s),
    )
    table_loads = [pltpu.make_async_copy(src, dst, table_sem.at[n]) for n, (src, dst) in enumerate(sources)]
    for c in table_loads:
        c.start()

    pl.semaphore_wait(barrier, peers - 1 + chs - 1)

    def rows_of(ref, g):
        return ref[:, :, lanes(g)].reshape(LAT_ROWS, SPAN).astype(f32)

    def put_rows(ref, g, value):
        ref[:, :, lanes(g)] = value.astype(bf16).reshape(32, 2, SPAN)

    def send_field(src, dst, kind, g):
        def go(p):
            pltpu.make_async_remote_copy(
                src_ref=src.at[p, :, lanes(g)],
                dst_ref=dst.at[lat, :, lanes(g)],
                send_sem=send_sem.at[kind, g],
                recv_sem=recv_sem.at[kind, g],
                device_id={"lat": p},
                device_id_type=MESH,
            ).start()

        each_peer(go)

    def wait_bytes(buf, sem):
        ref = buf.at[pl.ds(0, peers - 1)]
        pltpu.make_async_copy(ref, ref, sem).wait()

    def wait_field(buf, sem, kind, g):
        ref = buf.at[pl.ds(0, peers - 1), :, lanes(g)]
        pltpu.make_async_copy(ref, ref, sem.at[kind, g]).wait()

    def keep_own(src, dst, g):
        dst[lat, :, lanes(g)] = src[lat, :, lanes(g)]

    loads[0].wait()
    send_field(upr, cols.at[0], UP, 0)
    send_field(upr, cols.at[0], UP, 1)
    first[...] = jnp.zeros_like(first)
    second[...] = jnp.zeros_like(second)
    loads[1].wait()

    @pl.loop(0, GROUPS)
    def _(g):
        x = rows_of(tok, g)
        first[...] += x
        second[...] += x * x

    def rows8(p):
        return pl.ds(pl.multiple_of(p * 8, 8), 8)

    def over_channels(which):
        sums_send[which, :, 0:LON] = narrow(first)
        sums_send[which, :, LON : 2 * LON] = narrow(second)
        sums_send[which, :, 2 * LON :] = jnp.zeros((LAT_ROWS, 384 - 2 * LON), f32)
        sums_recv[which, ch] = sums_send[which, rows8(ch), :]

        def go(p):
            pltpu.make_async_remote_copy(
                src_ref=sums_send.at[which, rows8(p), :],
                dst_ref=sums_recv.at[which, ch],
                send_sem=ch_send.at[which],
                recv_sem=ch_recv.at[which],
                device_id={"ch": p},
                device_id_type=MESH,
            ).start()

        each_ch(go)

    def share_channels(which):
        ref = sums_recv.at[which, pl.ds(0, chs - 1)]
        pltpu.make_async_copy(ref, ref, ch_recv.at[which]).wait()
        total = sums_recv[which, 0]
        for p in range(1, chs):
            total = total + sums_recv[which, p]
        sums_all[which, ch] = total * (1.0 / EMBED)

        def go(p):
            pltpu.make_async_remote_copy(
                src_ref=sums_all.at[which, ch],
                dst_ref=sums_all.at[which, ch],
                send_sem=all_send.at[which],
                recv_sem=all_recv.at[which],
                device_id={"ch": p},
                device_id_type=MESH,
            ).start()

        each_ch(go)

    def wait_channels(which):
        ref = sums_all.at[which, pl.ds(0, chs - 1)]
        pltpu.make_async_copy(ref, ref, all_recv.at[which]).wait()
        return sums_all[which].reshape(LAT_ROWS, 384)

    over_channels(0)
    for c in table_loads:
        c.wait()

    @pl.loop(0, GROUPS)
    def _(g):
        for source, wide in ((gain_s, gain_x), (shift_s, shift_x)):
            for c in range(GROUP):
                wide[g, :, c * LON : (c + 1) * LON] = jnp.full((1, LON), source[g * GROUP + c], f32)

    share_channels(0)
    ya[...] = jnp.zeros_like(ya)
    yb[...] = jnp.zeros_like(yb)
    bias[...] = jnp.zeros_like(bias)
    for n, (w_ref, b_ref) in enumerate(((w1_ref, b1_ref), (w2_ref, b2_ref))):
        real, imag = w_ref[0, 0], w_ref[1, 0]
        big[:CH, :CH] = real
        big[CH:, CH:] = real
        big[:CH, CH:] = imag
        big[CH:, :CH] = -imag
        matrix = big[...]
        wt[n] = matrix.astype(bf16)
        wh[n], wl[n] = split(matrix.T)
        bias[n : n + 1, 0:CH] = b_ref[0]
        bias[n : n + 1, CH : 2 * CH] = b_ref[1]
    for g in range(GROUPS):
        keep_own(upr, cols.at[0], g)
    for r in (a1, a2, c1, c2, pack, parts):
        r[...] = jnp.zeros_like(r)
    bias_columns[...] = bias[...].T
    sums = wait_channels(0)
    mean = sums[:, 0:LON]
    variance = sums[:, LON : 2 * LON] - mean * mean
    widen(center, mean)
    widen(scale, lax.rsqrt(variance + layer_eps))

    @pl.loop(0, GROUPS)
    def _(g):
        standard = (rows_of(tok, g) - center[...]) * scale[...]
        put_rows(normed, g, standard * gain_x[g] + shift_x[g])
        keep_own(normed, cols.at[1], g)
        send_field(normed, cols.at[1], NORM, g)

    send_field(upr, cols.at[0], UP, 2)

    def spectrum(field, g):
        x = cols[field, :, :, lanes(g)].reshape(LAT_ROWS, SPAN)
        both = dot(lat_ref[...], x)
        zs[...] = both[:LAT_ROWS] + both[LAT_ROWS:]
        for c in range(GROUP):
            v = zs[:, c * LON : (c + 1) * LON]
            ya[pl.ds(c, LAT_ROWS, stride=PITCH), :] = v[:, :128]
            yb[pl.ds(c, LAT_ROWS, stride=PITCH), 0 : LON - 128] = v[:, 128:]
        rows = jnp.concatenate([ya[...], yb[...]], axis=1)
        rows = rows.reshape(LAT_ROWS, PITCH, 256)[:, :GROUP].reshape(LAT_ROWS * GROUP, 256)
        high, low = split(rows)
        p = dot(high, lonh[field]) + dot(low, lonh[field]) + dot(high, lonl[field])
        p = p.reshape(LAT_ROWS, GROUP, 256)
        cc, cs = p[:, :, :128], p[:, :, 128:]
        here = pl.ds(pl.multiple_of(g * GROUP, GROUP), GROUP)
        re, im = spec.at[field, 0], spec.at[field, 1]
        re[0:1, here] = cc[0:1]
        im[0:1, here] = -cs[0:1]
        re[32:33, here] = cc[32:33]
        im[32:33, here] = -cs[32:33]
        re[1:32, here] = cc[1:32] - cs[33:64]
        re[33:64, here] = cc[1:32] + cs[33:64]
        im[1:32, here] = -cs[1:32] - cc[33:64]
        im[33:64, here] = cc[33:64] - cs[1:32]

    @pl.loop(0, 2)
    def _(g):
        wait_field(cols.at[0], recv_sem, UP, g)
        spectrum(0, g)

    @pl.loop(0, GROUPS)
    def _(g):
        wait_field(cols.at[1], recv_sem, NORM, g)
        spectrum(1, g)

    @pl.loop(0, LAT_ROWS // STEP)
    def _(i):
        at = pl.ds(i * STEP, STEP)
        re, im = spec.at[1, 0], spec.at[1, 1]
        xh, xl = split(gather_modes(re[at], im[at]))
        pre = dot(wh[0], xh) + dot(wh[0], xl) + dot(wl[0], xh) + bias_columns[: 2 * CH, 0:1]
        a = math.sqrt(2.0 / math.pi)
        sq = pre * pre
        th = jnp.tanh(a * pre * (1.0 + 0.044715 * sq))
        half = 0.5 * (1.0 + th)
        hid = pre * half
        slope = half + 0.5 * pre * (1.0 - th * th) * (a * (1.0 + 3.0 * 0.044715 * sq))
        hh, hl = split(hid)
        pre2 = dot(wh[1], hh) + dot(wh[1], hl) + dot(wl[1], hh) + bias_columns[: 2 * CH, 1:2]
        t = jnp.tanh(pre2 * (1.0 / shrink))
        mixed = pre2 - shrink * t
        for j in range(STEP):
            re[i * STEP + j] = mixed[:CH, 128 * j : 128 * (j + 1)]
            im[i * STEP + j] = mixed[CH:, 128 * j : 128 * (j + 1)]
        stash[0, i] = xh
        stash[1, i] = slope.astype(bf16)
        stash[2, i] = hh
        stash[3, i] = (t * t).astype(bf16)

    def field_of(field, g):
        here = pl.ds(pl.multiple_of(g * GROUP, GROUP), GROUP)
        gr, gi = spec[field, 0, :, here], spec[field, 1, :, here]
        left = jnp.concatenate([gr[0:1], gr[1:32] + gr[33:64], gr[32:33], gi[33:64] - gi[1:32]], axis=0)
        right = -jnp.concatenate([gi[0:1], gi[1:32] + gi[33:64], gi[32:33], gr[1:32] - gr[33:64]], axis=0)
        rows = jnp.concatenate([left, right], axis=2).reshape(LAT_ROWS * GROUP, 256).astype(bf16)
        v = dot(rows, lonih[field]) + dot(rows, lonil[field])
        v = v.reshape(LAT_ROWS, GROUP, 256)
        va, vb = ya.reshape(LAT_ROWS, PITCH, 128), yb.reshape(LAT_ROWS, PITCH, 128)
        va[:, 0:GROUP, :] = v[:, :, :128]
        vb[:, 0:GROUP, :] = v[:, :, 128:]
        for c in range(GROUP):
            zs[:, c * LON : c * LON + 128] = ya[pl.ds(c, LAT_ROWS, stride=PITCH), :]
            zs[:, c * LON + 128 : (c + 1) * LON] = yb[pl.ds(c, LAT_ROWS, stride=PITCH), 0 : LON - 128]
        z = zs[...].astype(bf16)
        return dot(latih[...], z) + dot(latil[...], z)

    @pl.loop(0, GROUPS)
    def _(g):
        put_rows(away, g, field_of(1, g))
        keep_own(away, filt, g)
        send_field(away, filt, FILT, g)

    wait_field(cols.at[0], recv_sem, UP, 2)
    yb[:, LON - 128 :] = jnp.zeros((LAT_ROWS * PITCH, 256 - LON), f32)
    spectrum(0, 2)

    @pl.loop(0, LAT_ROWS // STEP)
    def _(i):
        at = pl.ds(i * STEP, STEP)
        re, im = spec.at[0, 0], spec.at[0, 1]
        p2 = gather_modes(re[at], im[at]) * stash[3, i].astype(f32)
        p2h = p2.astype(bf16)
        p1 = dot(wt[1], p2h) * stash[1, i].astype(f32)
        p1h = p1.astype(bf16)
        out = dot(wt[0], p1h)
        for j in range(STEP):
            re[i * STEP + j] = out[:CH, 128 * j : 128 * (j + 1)]
            im[i * STEP + j] = out[CH:, 128 * j : 128 * (j + 1)]
        a2[...] += dot_nt(stash[2, i], p2h)
        a1[...] += dot_nt(stash[0, i], p1h)
        c2[...] += sum(p2[:, 128 * j : 128 * (j + 1)] for j in range(STEP))
        c1[...] += sum(p1[:, 128 * j : 128 * (j + 1)] for j in range(STEP))

    for n, (acc, line) in enumerate(((a1, c1), (a2, c2))):
        v = acc[...]
        top = n * 2 * CH
        pack[top : top + CH, :CH] = v[:CH, :CH] + v[CH:, CH:]
        pack[top + CH : top + 2 * CH, :CH] = v[:CH, CH:] - v[CH:, :CH]
        row = jnp.sum(line[...].T, axis=0, keepdims=True)
        pack[4 * CH + 2 * n : 4 * CH + 2 * n + 1, :CH] = row[:, :CH]
        pack[4 * CH + 2 * n + 1 : 4 * CH + 2 * n + 2, :CH] = row[:, CH:]

    pack16[...] = pack[...].astype(bf16)

    def rows16(p):
        return pl.ds(pl.multiple_of(p * 16, 16), 16)

    packed_recv[lat] = pack16[rows16(lat), :]

    def send_piece(p):
        pltpu.make_async_remote_copy(
            src_ref=pack16.at[rows16(p), :],
            dst_ref=packed_recv.at[lat],
            send_sem=small_send.at[0],
            recv_sem=small_recv.at[0],
            device_id={"lat": p},
            device_id_type=MESH,
        ).start()

    each_peer(send_piece)

    first[...] = jnp.zeros_like(first)
    second[...] = jnp.zeros_like(second)

    @pl.loop(0, GROUPS)
    def _(g):
        out = field_of(0, g).astype(bf16)
        total = rows_of(cols.at[0], g) + out.astype(f32)
        first[...] += total * gain_x[g]
        second[...] += total * (rows_of(cols.at[1], g) - shift_x[g])
        put_rows(cols.at[0], g, out)
        keep_own(cols.at[0], grad, g)

        @pl.when(g < GROUPS - 1)
        def _():
            send_field(cols.at[0], grad, GRAD, g)

    over_channels(1)
    share_channels(1)
    mean_send[...] = wait_channels(1).reshape(32, 2, 384)
    mean_recv[lat] = mean_send[lat]

    def send_mean(p):
        pltpu.make_async_remote_copy(
            src_ref=mean_send.at[p],
            dst_ref=mean_recv.at[lat],
            send_sem=small_send.at[3],
            recv_sem=small_recv.at[3],
            device_id={"lat": p},
            device_id_type=MESH,
        ).start()

    each_peer(send_mean)
    send_field(cols.at[0], grad, GRAD, GROUPS - 1)

    @pl.loop(0, GROUPS)
    def _(g):
        wait_field(filt, recv_sem, FILT, g)
        put_rows(filt, g, rows_of(tok, g) + rows_of(normed, g) + rows_of(filt, g))
        pltpu.make_async_copy(filt.at[:, :, lanes(g)], result.at[:, :, lanes(g)], store_sem.at[0, g]).start()

    wait_bytes(packed_recv, small_recv.at[0])
    piece[...] = jnp.sum(packed_recv[...].astype(f32), axis=0).astype(bf16)
    params_out[lat] = piece[...]

    def send_sum(p):
        pltpu.make_async_remote_copy(
            src_ref=piece,
            dst_ref=params_out.at[lat],
            send_sem=small_send.at[1],
            recv_sem=small_recv.at[1],
            device_id={"lat": p},
            device_id_type=MESH,
        ).start()

    each_peer(send_sum)

    wait_bytes(mean_recv, small_recv.at[3])
    means = mean_recv[...].reshape(LAT_ROWS, 384)
    widen(first, means[:, 0:LON])
    widen(second, means[:, LON : 2 * LON])

    def close_part(g):
        base = parts[:, g * SPAN : (g + 1) * SPAN]
        column = jnp.concatenate(
            [jnp.sum(base[:, c * LON : (c + 1) * LON], axis=1, keepdims=True) for c in range(GROUP)], axis=1
        )
        ends_send[:, g * GROUP : (g + 1) * GROUP] = column[0:2]

    ends_send[...] = jnp.zeros_like(ends_send)

    def sum_part(g):
        standard = (rows_of(tok, g) - center[...]) * scale[...]
        total = rows_of(upr, g) + rows_of(grad, g)
        parts[0:1, lanes(g)] = jnp.sum(total * standard, axis=0, keepdims=True)
        parts[1:2, lanes(g)] = jnp.sum(total, axis=0, keepdims=True)

    def finish_tokens(g):
        inverse = scale[...]
        standard = (rows_of(tok, g) - center[...]) * inverse
        up = rows_of(upr, g)
        slope = (up + rows_of(grad, g)) * gain_x[g]
        put_rows(grad, g, up + inverse * (slope - first[...] - standard * second[...]))
        pltpu.make_async_copy(grad.at[:, :, lanes(g)], grad_tokens.at[:, :, lanes(g)], store_sem.at[1, g]).start()

    def send_ends(p):
        pltpu.make_async_remote_copy(
            src_ref=ends_send,
            dst_ref=ends_recv.at[lat],
            send_sem=small_send.at[2],
            recv_sem=small_recv.at[2],
            device_id={"lat": p},
            device_id_type=MESH,
        ).start()

    @pl.loop(0, GROUPS)
    def _(g):
        wait_field(grad, recv_sem, GRAD, g)
        sum_part(g)
        for k in range(GROUPS):
            pl.when(g == k)(functools.partial(close_part, k))

        @pl.when(g == GROUPS - 1)
        def _():
            ends_recv[lat] = ends_send[...]
            each_peer(send_ends)

        finish_tokens(g)

    wait_bytes(ends_recv, small_recv.at[2])
    ends_out[...] = jnp.sum(ends_recv[...], axis=0)
    wait_bytes(params_out, small_recv.at[1])
    for which, buf, out in ((0, filt, result), (1, grad, grad_tokens)):
        for g in range(GROUPS):
            pltpu.make_async_copy(buf.at[:, :, lanes(g)], out.at[:, :, lanes(g)], store_sem.at[which, g]).wait()
    for kind, buf in ((UP, upr), (NORM, normed), (FILT, away), (GRAD, cols.at[0])):
        for g in range(GROUPS):
            wait_field(buf, send_sem, kind, g)
    for which in range(2):
        ref = sums_recv.at[which, pl.ds(0, chs - 1)]
        pltpu.make_async_copy(ref, ref, ch_send.at[which]).wait()
        ref = sums_all.at[which, pl.ds(0, chs - 1)]
        pltpu.make_async_copy(ref, ref, all_send.at[which]).wait()
    wait_bytes(packed_recv, small_send.at[0])
    wait_bytes(params_out, small_send.at[1])
    wait_bytes(ends_recv, small_send.at[2])
    wait_bytes(mean_recv, small_send.at[3])


PIECES = 9


def finish_kernel(
    result, grad_tokens, params, ends, o_result, o_grad, o_fw, o_fb, o_sw, o_sb, o_og, o_os,
    hold, params_v, ends_v, fw, fb, sw, sb, og, os, load_sem, store_sem, small_load, small_store,
):
    width = CH * LON // PIECES
    pairs = ((result, o_result), (grad_tokens, o_grad))
    at = lambda ref, i: ref.at[:, :, i * width : (i + 1) * width]
    small = [
        pltpu.make_async_copy(params, params_v, small_load.at[0]),
        pltpu.make_async_copy(ends, ends_v, small_load.at[1]),
    ]
    loads = [
        [pltpu.make_async_copy(at(src, i), at(hold.at[n], i), load_sem.at[n, i]) for n, (src, _) in enumerate(pairs)]
        for i in range(PIECES)
    ]
    stores = [
        [pltpu.make_async_copy(at(hold.at[n], i), at(dst, i), store_sem.at[n, i]) for n, (_, dst) in enumerate(pairs)]
        for i in range(PIECES)
    ]
    for c in small + sum(loads, []):
        c.start()
    for c in small:
        c.wait()
    p = params_v[...].astype(f32).reshape(512, 128)
    for n, (weight, line) in enumerate(((fw, fb), (sw, sb))):
        for part in range(2):
            top = (2 * n + part) * CH
            weight[part, 0] = p[top : top + CH, :CH]
            line[part] = p[4 * CH + 2 * n + part : 4 * CH + 2 * n + part + 1, :CH]
    og[...] = ends_v[0:1, :CH]
    os[...] = ends_v[1:2, :CH]
    outs = ((fw, o_fw), (fb, o_fb), (sw, o_sw), (sb, o_sb), (og, o_og), (os, o_os))
    small = [pltpu.make_async_copy(src, dst, small_store.at[n]) for n, (src, dst) in enumerate(outs)]
    for c in small:
        c.start()
    for i in range(PIECES):
        for n in range(2):
            loads[i][n].wait()
            stores[i][n].start()
    for c in small + sum(stores, []):
        c.wait()


def finish(result, grad_tokens, params, ends):
    hbm = pl.BlockSpec(memory_space=pl.ANY)
    field = jax.ShapeDtypeStruct((32, 2, CH * LON), bf16)
    weight, line, vec = [jax.ShapeDtypeStruct(x, f32) for x in ((2, 1, CH, CH), (2, 1, CH), (1, CH))]
    small = [weight, line, weight, line, vec, vec]
    return pl.pallas_call(
        finish_kernel,
        in_specs=[hbm] * 4,
        out_specs=[hbm] * 8,
        out_shape=[field, field] + small,
        scratch_shapes=[
            pltpu.VMEM((2, 32, 2, CH * LON), bf16),
            *[pltpu.VMEM(x.shape, x.dtype) for x in (params, ends, *small)],
            pltpu.SemaphoreType.DMA((2, PIECES)), pltpu.SemaphoreType.DMA((2, PIECES)),
            pltpu.SemaphoreType.DMA((2,)), pltpu.SemaphoreType.DMA((6,)),
        ],
        compiler_params=pltpu.CompilerParams(vmem_limit_bytes=67_043_328),
        name="finish",
    )(result, grad_tokens, params, ends)


def mega(gain, shift, tokens, upstream, w1, b1, w2, b2):
    lat, lon, lon2 = tables()
    pair = lambda a, b: [jnp.asarray(np.stack(x)) for x in zip(split_table(a), split_table(b))]
    lat_h, lat_l = split_table(lat)
    lati_h, lati_l = split_table(lat.T)
    lonh, lonl = pair(lon2, lon)
    lonih, lonil = pair(lon.T, lon2.T)
    hbm, vmem = pl.BlockSpec(memory_space=pl.ANY), pl.BlockSpec(memory_space=pltpu.VMEM)
    field = jax.ShapeDtypeStruct((32, 2, CH * LON), bf16)
    V, D = pltpu.VMEM, pltpu.SemaphoreType.DMA
    fld = V((32, 2, CH * LON), bf16)
    wide = V((LAT_ROWS, SPAN), f32)
    ins = [
        gain, shift, tokens, upstream, w1, b1, w2, b2,
        jnp.asarray(np.concatenate([lat_h, lat_l], axis=0)), lonh, lonl,
        jnp.asarray(lati_h), jnp.asarray(lati_l), lonih, lonil,
    ]
    return pl.pallas_call(
        mega_kernel,
        in_specs=[hbm] * len(ins),
        out_specs=[hbm, hbm, vmem, vmem],
        out_shape=[
            field, field,
            jax.ShapeDtypeStruct((32, 16, 128), bf16),
            jax.ShapeDtypeStruct((2, 128), f32),
        ],
        scratch_shapes=[
            *[V(x.shape, x.dtype) for x in ins[4:]], pltpu.SMEM((CH,), f32), pltpu.SMEM((CH,), f32), D((len(ins) - 2,)),
            V((GROUPS, 1, SPAN), f32), V((GROUPS, 1, SPAN), f32), V((192, 192), f32), V((8, 256), f32), V((256, 8), f32),
            fld, fld, V((2, 32, 2, CH * LON), bf16), fld, fld, fld, fld,
            V((2, 2, LAT_ROWS, CH, 128), f32),
            V((4, LAT_ROWS // STEP, 2 * CH, 128 * STEP), bf16),
            wide, V((LAT_ROWS * PITCH, 128), f32), V((LAT_ROWS * PITCH, 128), f32),
            wide, wide, wide, wide,
            V((2, LAT_ROWS, 384), f32), V((2, 8, 8, 384), f32), V((2, 8, 8, 384), f32),
            V((2, 192, 192), bf16), V((2, 192, 192), bf16), V((2, 192, 192), bf16),
            V((192, 192), f32), V((192, 192), f32), V((192, 128), f32), V((192, 128), f32),
            V((512, 128), f32), V((512, 128), bf16), V((32, 16, 128), bf16), V((16, 128), bf16),
            V((8, CH * LON), f32), V((2, 128), f32), V((32, 2, 128), f32), V((32, 2, 384), f32), V((32, 2, 384), f32),
            D((2,)), D((2, GROUPS)), D((4, GROUPS)), D((4, GROUPS)), D((2,)), D((2,)), D((2,)), D((2,)), D((4,)), D((4,)),
        ],
        compiler_params=pltpu.CompilerParams(
            collective_id=0, has_side_effects=True, vmem_limit_bytes=67_043_328
        ),
        name="afno",
    )(*ins)


def body(
    tokens, norm_gain, norm_shift, first_weight, first_bias, second_weight, second_bias, upstream
):
    ends = mega(
        norm_gain, norm_shift, tokens, upstream, first_weight, first_bias, second_weight, second_bias
    )
    result, grad_tokens, fw, fb, sw, sb, gain, shift = finish(*ends)
    return result, grad_tokens, fw, fb, sw, sb, gain.reshape(CH), shift.reshape(CH)


def solution(mesh):
    whole, weight, bias = P(None, "lat", "ch"), P(None, "ch", None, None), P(None, "ch", None)
    return jax.shard_map(
        body,
        mesh=mesh,
        in_specs=(whole, P("ch"), P("ch"), weight, bias, weight, bias, whole),
        out_specs=(whole, whole, weight, bias, weight, bias, P("ch"), P("ch")),
        check_vma=False,
    )
```
